128 devices in a mesh: gx: 4 (over y), gy: 8 (over x, core), gz: 4 (over z).
Axes of the slice: x: 4, y: 4, z: 4, core: 2. Of those that a mesh axis runs over, the one named last changes fastest.
Arguments:
- rhs: float32 [8, 64, 256, 512], P(None, 'gx', 'gy', 'gz'), may hold values from -8 to 8
- stencil: float32 [14, 64, 256, 512], P(None, 'gx', 'gy', 'gz'), may hold values from 0.02 to 1
Outputs:
- solution: float32 [8, 64, 256, 512], P(None, 'gx', 'gy', 'gz')
- residual: float32 [8, 64, 256, 512], P(None, 'gx', 'gy', 'gz')
The draws below stay inside these ranges and needn't reach their ends.
All inputs are finite; a program needn't handle non-finite values.
Results may differ from the reference program's by a relative error of at most 0.00029.
Values sent between devices are 32-bit elements; how exact they have to be, the bound alone decides.
A program may use at most 128 MiB of HBM per device.

```python
import math
import jax
import jax.numpy as jnp
from jax import lax

NRHS = 8
ITERS = 2
NX = 64
NY = 256
NZ = 512


def block_levels(own_key, dims, shards, low, high):
    level = 1.0
    for dim, blocks in shards:
        steps = jax.random.uniform(jax.random.fold_in(jax.random.fold_in(own_key, 6), dim), (blocks,), jnp.float32, low / len(shards), high / len(shards))
        level = level * jnp.repeat(jnp.exp(steps), dims[dim] // blocks).reshape((-1,) + (1,) * (len(dims) - 1 - dim))
    return level


def bell_draw(rng, shape, scale, bound, split=(), dtype=jnp.bfloat16):
    level = block_levels(rng, shape, split, -0.22, 0.18) if split else 1.0
    values = jax.random.normal(rng, shape, jnp.float32) * scale * level
    return jnp.minimum(jnp.maximum(values, -bound), bound).astype(dtype)


def setup_inputs(seed: int = 0) -> dict:
    seeds = jax.random.split(jax.random.key(seed), 3)
    return {
        "rhs": bell_draw(seeds[0], (NRHS, NX, NY, NZ), 1.0, 8.0, ((1, 4), (2, 8), (3, 4)), jnp.float32),
        "stencil": jnp.clip(jnp.exp(math.log(1.0) - 3.912023 * jax.random.uniform(seeds[1], (14, NX, NY, NZ), jnp.float32) ** block_levels(seeds[1], (14, NX, NY, NZ), ((1, 4), (2, 8), (3, 4)), -0.2, 0.2)), 0.02, 1.0),
    }


FORWARD = [(a, b, c) for a in (-1, 0, 1) for b in (-1, 0, 1) for c in (-1, 0, 1) if (a, b, c) > (0, 0, 0)]

def window(array, margin, depth, offset):
    result = array
    for place in range(3):
        dim = array.ndim - 3 + place
        inner = array.shape[dim] - 2 * margin
        begin = margin - depth + offset[place]
        result = lax.slice_in_dim(result, begin, begin + inner + 2 * depth, axis=dim)
    return result

def diagonal_field(padded, margin, depth):
    total = window(padded[0], margin, depth, (0, 0, 0))
    total = total + jnp.sum(window(padded[1:], margin, depth, (0, 0, 0)), axis=0)
    for index, offset in enumerate(FORWARD):
        back = (-offset[0], -offset[1], -offset[2])
        total = total + window(padded[index + 1], margin, depth, back)
    return total

def operate(field, fmargin, padded, smargin, diag, depth):
    result = diag[None] * window(field, fmargin, depth, (0, 0, 0))
    for index, offset in enumerate(FORWARD):
        back = (-offset[0], -offset[1], -offset[2])
        ahead_w = window(padded[index + 1], smargin, depth, (0, 0, 0))
        behind_w = window(padded[index + 1], smargin, depth, back)
        result = result - ahead_w[None] * window(field, fmargin, depth, offset)
        result = result - behind_w[None] * window(field, fmargin, depth, back)
    return result

def gram(left, right):
    flat_l = left.reshape(left.shape[0], -1)
    flat_r = right.reshape(right.shape[0], -1)
    return lax.dot_general(flat_l.astype(jnp.float32), flat_r.astype(jnp.float32), (((1,), (1,)), ((), ())), precision=lax.Precision.HIGHEST, preferred_element_type=jnp.float32)

def combine(coef, field):
    return jnp.einsum('ij,ixyz->jxyz', coef, field, precision=lax.Precision.HIGHEST)

def solve_spd(matrix, right):
    factor = jnp.linalg.cholesky(matrix)
    return jax.scipy.linalg.cho_solve((factor, True), right)

def reference(rhs, stencil):
    padded = jnp.pad(stencil, ((0, 0), (1, 1), (1, 1), (1, 1)))
    diag = diagonal_field(padded, 1, 0)
    solution = jnp.zeros_like(rhs)
    residual = rhs
    direction = rhs
    norm_now = gram(residual, residual)
    for step in range(ITERS):
        field = jnp.pad(direction, ((0, 0), (1, 1), (1, 1), (1, 1)))
        image = operate(field, 1, padded, 1, diag, 0)
        alpha = solve_spd(gram(direction, image), norm_now)
        solution = solution + combine(alpha, direction)
        residual = residual - combine(alpha, image)
        if step + 1 < ITERS:
            norm_next = gram(residual, residual)
            beta = solve_spd(norm_now, norm_next)
            direction = residual + combine(beta, direction)
            norm_now = norm_next
    return (solution, residual)
```

```python
import functools

import jax
import jax.numpy as jnp
from jax import lax
from jax.experimental import pallas as pl
from jax.experimental.pallas import tpu as pltpu
from jax.sharding import PartitionSpec as P

F32 = jnp.float32
N = 8
FORWARD = [
    (a, b, c) for a in (-1, 0, 1) for b in (-1, 0, 1) for c in (-1, 0, 1) if (a, b, c) > (0, 0, 0)
]
INDEX = {o: k + 1 for k, o in enumerate(FORWARD)}
PLANE = [(a, b) for a in (-1, 0, 1) for b in (-1, 0, 1)]
SLOTS = [(0, 0), (0, 1), (1, -1), (1, 0), (1, 1)]
LOW = [INDEX[(a, b, 1)] for a, b in SLOTS]
UP = [INDEX[(a, b, -1)] if (a, b) != (0, 0) else INDEX[(0, 0, 1)] for a, b in SLOTS]
DIRS = [
    (a, b, c) for a in (-1, 0, 1) for b in (-1, 0, 1) for c in (-1, 0, 1) if (a, b, c) != (0, 0, 0)
]
WRANGE = {(1, 0): (5, 9), (1, 1): (11, 3), (1, -1): (5, 3), (0, 1): (2, 12), (0, -1): (5, 3)}
WDIRS = list(WRANGE)
PAIRS = [(i, j) for i in range(N) for j in range(i, N)]
TOP = 8


def lanes():
    return lax.broadcasted_iota(jnp.int32, (8, 128), 1)


def rows():
    return lax.broadcasted_iota(jnp.int32, (8, 128), 0)


def splat_row(m, k):
    return jnp.broadcast_to(m[k : k + 1, :], (8, 128))


def splat_col(m, k):
    return jnp.broadcast_to(m[:, k : k + 1], (8, 128))


def row_sum(m):
    return jnp.broadcast_to(jnp.sum(m, axis=1, keepdims=True), (8, 128))


def shift(m, amount):
    amount = amount % 128
    return pltpu.roll(m, amount, 1) if amount else m


def product(a, b):
    total = splat_col(a, 0) * splat_row(b, 0)
    for k in range(1, N):
        total = total + splat_col(a, k) * splat_row(b, k)
    return total


def product_t(a, b):
    same = lanes() == rows()
    total = None
    for k in range(N):
        column = row_sum(jnp.where(same, splat_row(a, k), 0.0))
        term = column * splat_row(b, k)
        total = term if total is None else total + term
    return total


def eliminate(m):
    row_id = rows()
    for k in range(N):
        pivot = splat_row(m, k)
        scaled = pivot / splat_col(pivot, k)
        m = jnp.where(row_id == k, scaled, m - splat_col(m, k) * scaled)
    return m


def pack_lanes(parts):
    lane = lanes()
    total = None
    for slot, part in enumerate(parts):
        here = (lane >= 8 * slot) & (lane < 8 * slot + 8)
        term = jnp.where(here, shift(part, 8 * slot), 0.0)
        total = term if total is None else total + term
    return total


def kernel(
    sizes,
    x_ref,
    w_ref,
    q_out,
    s_out,
    c_out,
    V,
    Q,
    W,
    WW,
    WE,
    R,
    PP,
    LPP,
    PQ,
    LPQ,
    G,
    GW,
    S,
    ARS,
    ARL,
    load_sem,
    out_sem,
    send1,
    recv1,
    send2,
    recv2,
    ar_send,
    ar_recv,
):
    names = ("gx", "gy", "gz")
    nx, ny, nz = sizes
    me = tuple(lax.axis_index(n) for n in names)

    def exists(d):
        cond = None
        for pos, step, count in zip(me, d, sizes):
            term = None
            if step > 0:
                term = pos < count - 1
            elif step < 0:
                term = pos > 0
            if term is not None:
                cond = term if cond is None else cond & term
        return cond

    def opposite(d):
        return tuple(-t for t in d)

    def target(d):
        return tuple(pos + step for pos, step in zip(me, d))

    def peer(axis, p):
        return tuple(
            lax.rem(pos + p, sizes[i]) if i == axis else pos for i, pos in enumerate(me)
        )

    load_x = pltpu.make_async_copy(x_ref, V.at[:, pl.ds(1, 16), pl.ds(TOP, 32)], load_sem.at[0])
    load_w = pltpu.make_async_copy(w_ref, W.at[:, pl.ds(1, 16), pl.ds(TOP, 32)], load_sem.at[1])
    load_x.start()
    load_w.start()

    zero = jnp.zeros((8, 128), F32)

    def clear_padded(buf, first, last):
        for field in range(buf.shape[0]):
            for plane in (first, last):
                if plane is not None:
                    for t in range(6):
                        buf[field, plane, pl.ds(8 * t, 8)] = zero

        def body(p, carry):
            for field in range(buf.shape[0]):
                buf[field, p, pl.ds(0, 8)] = zero
                buf[field, p, pl.ds(40, 8)] = zero
            return carry

        lax.fori_loop(1, 17, body, 0)

    clear_padded(V, 0, 17)
    clear_padded(Q, 0, 17)
    clear_padded(W, 0, None)

    def clear_landing(i, carry):
        for t in range(6):
            for s in range(2):
                for k in range(2):
                    LPP[s, k, i, pl.ds(8 * t, 8)] = zero
                LPQ[s, i, pl.ds(8 * t, 8)] = zero
        return carry

    lax.fori_loop(0, 4, clear_landing, 0)

    barrier = pltpu.get_barrier_semaphore()
    for d in DIRS:

        @pl.when(exists(d))
        def _():
            pl.semaphore_signal(
                barrier, inc=1, device_id=target(d), device_id_type=pl.DeviceIdType.MESH
            )

    for axis in range(3):
        for p in range(1, sizes[axis]):
            pl.semaphore_signal(
                barrier, inc=1, device_id=peer(axis, p), device_id_type=pl.DeviceIdType.MESH
            )
    span = []
    for pos, count in zip(me, sizes):
        span.append(1 + (pos > 0).astype(jnp.int32) + (pos < count - 1).astype(jnp.int32))
    pl.semaphore_wait(
        barrier, span[0] * span[1] * span[2] - 1 + (nx - 1) + (ny - 1) + (nz - 1)
    )

    def along(step, whole, plus, minus):
        if step == 0:
            return (pl.ds(*whole), pl.ds(*whole))
        src, dst = plus if step > 0 else minus
        return (pl.ds(src, 1), pl.ds(dst, 1))

    def field_part(d, buf, sends, recvs):
        i = DIRS.index(d)
        xs, xd = along(d[0], (1, 16), (16, 0), (1, 17))
        ys, yd = along(d[1], (TOP, 32), (TOP + 31, TOP - 1), (TOP, TOP + 32))
        return pltpu.make_async_remote_copy(
            src_ref=buf.at[:, xs, ys],
            dst_ref=buf.at[:, xd, yd],
            send_sem=sends.at[i],
            recv_sem=recvs.at[i],
            device_id=target(d),
            device_id_type=pl.DeviceIdType.MESH,
        )

    def weight_part(d):
        i = 26 + WDIRS.index((d[0], d[1]))
        k0, kn = WRANGE[(d[0], d[1])]
        xs, xd = along(d[0], (1, 16), (16, 0), (1, 17))
        ys, yd = along(d[1], (TOP, 32), (TOP + 31, TOP - 1), (TOP, TOP + 32))
        return pltpu.make_async_remote_copy(
            src_ref=W.at[pl.ds(k0, kn), xs, ys],
            dst_ref=W.at[pl.ds(k0, kn), xd, yd],
            send_sem=send1.at[i],
            recv_sem=recv1.at[i],
            device_id=target(d),
            device_id_type=pl.DeviceIdType.MESH,
        )

    def column_part(d, both):
        i = DIRS.index(d)
        side = 0 if d[2] > 0 else 1
        if d[0] == 0:
            gs, gd = pl.ds(0, 2), pl.ds(1, 2)
        elif d[0] > 0:
            gs, gd = pl.ds(1, 1), pl.ds(0, 1)
        else:
            gs, gd = pl.ds(0, 1), pl.ds(3, 1)
        if d[1] == 0:
            ys, yd = pl.ds(0, 32), pl.ds(TOP, 32)
        elif d[1] > 0:
            ys, yd = pl.ds(31, 1), pl.ds(TOP - 1, 1)
        else:
            ys, yd = pl.ds(0, 1), pl.ds(TOP + 32, 1)
        src = PP.at[:, gs, ys] if both else PQ.at[gs, ys]
        dst = LPP.at[side, :, gd, yd] if both else LPQ.at[side, gd, yd]
        return pltpu.make_async_remote_copy(
            src_ref=src,
            dst_ref=dst,
            send_sem=(send1 if both else send2).at[i],
            recv_sem=(recv1 if both else recv2).at[i],
            device_id=target(d),
            device_id_type=pl.DeviceIdType.MESH,
        )

    def start_if(d, copy):
        @pl.when(exists(d))
        def _():
            copy.start()

    def recv_if(d, copy):
        @pl.when(exists(opposite(d)))
        def _():
            copy.wait_recv()

    def sent_if(d, copy):
        @pl.when(exists(d))
        def _():
            copy.wait_send()

    flat = sorted((d for d in DIRS if d[2] == 0), key=lambda d: abs(d[1]))
    flat_w = [(a, b, 0) for a, b in WDIRS]
    cols = [d for d in DIRS if d[2] != 0]

    lane = lanes()
    odd = lax.rem(lane, 2) == 1
    first = lane == 0
    last = lane == 127
    half = lane // 2

    def pack_fields(buf, dst):
        def body(i, carry):
            xg = i // 4
            yt = lax.rem(i, 4)
            r0 = pl.multiple_of(8 * yt, 8)
            total = zero
            for xm in range(8):
                for f in range(N):
                    v = buf[f, xg * 8 + xm + 1, pl.ds(r0 + TOP, 8)]
                    total = jnp.where(
                        half == 8 * xm + f, shift(v, 16 * xm + 2 * f + 1), total
                    )
            dst(xg, r0, total)
            return carry

        lax.fori_loop(0, 8, body, 0)

    def pack_weights():
        def body(i, carry):
            xg = i // 4
            yt = lax.rem(i, 4)
            r0 = pl.multiple_of(8 * yt, 8)
            total = zero
            for xm in range(8):
                for j in range(5):
                    lo = W[LOW[j], xg * 8 + xm + 1, pl.ds(r0 + TOP, 8)]
                    up = W[UP[j], xg * 8 + xm + 1, pl.ds(r0 + TOP, 8)]
                    v = jnp.where(first, up, lo)
                    total = jnp.where(
                        half == 8 * xm + j, shift(v, 16 * xm + 2 * j + 1), total
                    )
            PP[1, xg, pl.ds(r0, 8)] = total
            return carry

        lax.fori_loop(0, 8, body, 0)

    def unpack(get, dst, planes):
        def body(t, carry):
            r0 = pl.multiple_of(8 * t, 8)
            merged = {}
            for xi in range(planes):
                if xi == 0:
                    g, off = 0, 112
                elif xi == 17:
                    g, off = 3, 0
                else:
                    g, off = 1 + (xi - 1) // 8, 16 * ((xi - 1) % 8)
                if g not in merged:
                    merged[g] = jnp.where(odd, get(1, g, r0), get(0, g, r0))
                dst[xi, pl.ds(r0, 8)] = shift(merged[g], -off)
            return carry

        lax.fori_loop(0, 6, body, 0)

    load_x.wait()
    for d in flat:
        start_if(d, field_part(d, V, send1, recv1))

    def put_pp(xg, r0, total):
        PP[0, xg, pl.ds(r0, 8)] = total

    pack_fields(V, put_pp)
    load_w.wait()
    for d in flat_w:
        start_if(d, weight_part(d))
    pack_weights()
    for d in cols:
        start_if(d, column_part(d, True))

    def gram_loop(get):
        def body(x, acc):
            acc = list(acc)
            for t in range(4):
                left, right = get(x, t)
                for n, (i, j) in enumerate(PAIRS):
                    acc[n] = acc[n] + left[i] * right[j]
            return tuple(acc)

        return lax.fori_loop(0, 16, body, tuple(zero for _ in PAIRS))

    def spread(parts, acc, offset):
        for n, (i, j) in enumerate(PAIRS):
            total = row_sum(acc[n])
            parts[i] = jnp.where(lane == offset + j, total, parts[i])
            if i != j:
                parts[j] = jnp.where(lane == offset + i, total, parts[j])
        return parts

    def fold(parts):
        result = zero
        for i in range(N):
            total = jnp.broadcast_to(jnp.sum(parts[i], axis=0, keepdims=True), (8, 128))
            result = jnp.where(rows() == i, total, result)
        return result

    def tile(buf, x, t):
        return [buf[f, x + 1, pl.ds(TOP + 8 * t, 8)] for f in range(N)]

    def get_rr(x, t):
        v = tile(V, x, t)
        return v, v

    parts1 = spread([zero] * N, gram_loop(get_rr), 0)

    for d in flat:
        recv_if(d, field_part(d, V, send1, recv1))
    for d in flat_w:
        recv_if(d, weight_part(d))
    for d in cols:
        recv_if(d, column_part(d, True))

    unpack(lambda s, g, r0: LPP[s, 0, g, pl.ds(r0, 8)], G, 18)
    unpack(lambda s, g, r0: LPP[s, 1, g, pl.ds(r0, 8)], GW, 17)

    def m_of(a, b):
        return 3 * (a + 1) + (b + 1)

    def prepare(x, carry):
        for t in range(4):
            r0 = TOP + 8 * t

            def w_at(k, a=0, b=0):
                return W[k, x + 1 + a, pl.ds(r0 + b, 8)]

            out = pl.ds(8 * t, 8)
            own = [w_at(k) for k in range(14)]
            diag = own[0]
            for k in range(1, 14):
                diag = diag + own[k]
            ahead = zero
            behind = zero
            edge = zero
            for j, (a, b) in enumerate(SLOTS):
                halo_w = GW[x + 1 - a, pl.ds(r0 - b, 8)]
                if (a, b) == (0, 0):
                    lo_here = splat_col(halo_w, 0)
                    WE[m_of(0, 0), x, out] = -jnp.where(odd, splat_col(own[1], 127), lo_here)
                    edge = edge + jnp.where(odd, 0.0, lo_here)
                else:
                    kf = INDEX[(a, b, 0)]
                    WE[m_of(a, b), x, out] = -jnp.where(
                        odd, splat_col(own[LOW[j]], 127), splat_col(own[UP[j]], 0)
                    )
                    back = jnp.where(
                        odd, splat_col(halo_w, 2 * j + 1), splat_col(halo_w, 2 * j)
                    )
                    WE[m_of(-a, -b), x, out] = -back
                    edge = edge + back
                    WW[m_of(a, b), x, out] = -own[kf]
                    flat_back = w_at(kf, -a, -b)
                    diag = diag + flat_back
                    WW[m_of(-a, -b), x, out] = -flat_back
                    up_back = w_at(UP[j], -a, -b)
                    ahead = ahead + up_back
                    WW[9 + m_of(-a, -b), x, out] = -up_back
                    WW[18 + m_of(a, b), x, out] = -shift(own[UP[j]], 127)
                WW[9 + m_of(a, b), x, out] = -shift(own[LOW[j]], 1)
                lo_back = w_at(LOW[j], -a, -b)
                behind = behind + lo_back
                WW[18 + m_of(-a, -b), x, out] = -lo_back
            diag = diag + jnp.where(last, edge, shift(ahead, 127))
            diag = diag + jnp.where(first, edge, shift(behind, 1))
            WW[m_of(0, 0), x, out] = diag
        return carry

    lax.fori_loop(0, 16, prepare, 0)

    def edges():
        def body(x, carry):
            for t in range(4):
                total = zero
                for a, b in PLANE:
                    total = total + WE[m_of(a, b), x, pl.ds(8 * t, 8)] * G[
                        x + 1 + a, pl.ds(TOP + 8 * t + b, 8)
                    ]
                R[x, pl.ds(8 * t, 8)] = total
            return carry

        lax.fori_loop(0, 16, body, 0)

    def operate(src, put):
        def body(x, carry):
            for t in range(4):
                at = pl.ds(8 * t, 8)
                weights = [WW[m, x, at] for m in range(27)]
                halo = R[x, at]
                for f in range(N):
                    sums = [None, None, None]
                    for m, (a, b) in enumerate(PLANE):
                        v = src[f, x + 1 + a, pl.ds(TOP + 8 * t + b, 8)]
                        for c in range(3):
                            term = weights[9 * c + m] * v
                            sums[c] = term if sums[c] is None else sums[c] + term
                    side = shift(halo, -(2 * f + 1))
                    total = sums[0] + shift(jnp.where(first, side, sums[1]), 127)
                    total = total + shift(jnp.where(last, side, sums[2]), 1)
                    put(f, x, t, total)
            return carry

        lax.fori_loop(0, 16, body, 0)

    def put_q(f, x, t, value):
        Q[f, x + 1, pl.ds(TOP + 8 * t, 8)] = value

    def put_s(f, x, t, value):
        S[f, x, pl.ds(8 * t, 8)] = value

    edges()
    operate(V, put_q)

    for d in flat:
        start_if(d, field_part(d, Q, send2, recv2))

    def put_pq(xg, r0, total):
        PQ[xg, pl.ds(r0, 8)] = total

    pack_fields(Q, put_pq)
    for d in cols:
        start_if(d, column_part(d, False))
    store_q = pltpu.make_async_copy(Q.at[:, pl.ds(1, 16), pl.ds(TOP, 32)], q_out, out_sem.at[0])
    store_q.start()

    axes = (1, 0, 2)
    base = {1: 0, 0: ny, 2: ny + nx}

    def reduce_copies(which, axis):
        copies = []
        for p in range(1, sizes[axis]):
            i = base[axis] + p
            copies.append(
                pltpu.make_async_remote_copy(
                    src_ref=ARS.at[which, axis],
                    dst_ref=ARL.at[which, base[axis] + me[axis]],
                    send_sem=ar_send.at[which, i],
                    recv_sem=ar_recv.at[which, i],
                    device_id=peer(axis, p),
                    device_id_type=pl.DeviceIdType.MESH,
                )
            )
        return copies

    def reduce_start(which, axis, value):
        ARS[which, axis] = value
        ARL[which, base[axis] + me[axis]] = value
        for copy in reduce_copies(which, axis):
            copy.start()

    def reduce_finish(which, axis):
        for copy in reduce_copies(which, axis):
            copy.wait_recv()
        total = ARL[which, base[axis]]
        for i in range(1, sizes[axis]):
            total = total + ARL[which, base[axis] + i]
        return total

    def trace_body(x, acc):
        acc = list(acc)
        for t in range(4):
            r, q = tile(V, x, t), tile(Q, x, t)
            for f in range(N):
                acc[f % 4] = acc[f % 4] + r[f] * q[f]
        return tuple(acc)

    tr = lax.fori_loop(0, 16, trace_body, (zero,) * 4)
    traced = row_sum((tr[0] + tr[1]) + (tr[2] + tr[3]))
    parts1[0] = jnp.where(lane == 8, traced, parts1[0])
    reduce_start(0, axes[0], fold(parts1))

    for d in flat:
        recv_if(d, field_part(d, Q, send2, recv2))
    reduce_start(0, axes[1], reduce_finish(0, axes[0]))
    for d in cols:
        recv_if(d, column_part(d, False))

    unpack(lambda s, g, r0: LPQ[s, g, pl.ds(r0, 8)], G, 18)
    edges()
    reduce_start(0, axes[2], reduce_finish(0, axes[1]))
    operate(Q, put_s)
    store_s = pltpu.make_async_copy(S, s_out, out_sem.at[1])
    store_s.start()
    sum1 = reduce_finish(0, axes[2])

    own_gram = jnp.where(lane < 8, sum1, 0.0)
    norm = jnp.sum(row_sum(jnp.where(lane == rows(), own_gram, 0.0)), axis=0, keepdims=True)
    theta = jnp.broadcast_to(splat_row(splat_col(sum1, 8), 0), (8, 128)) / jnp.broadcast_to(
        norm, (8, 128)
    )

    def get_h1(x, t):
        r, q = tile(V, x, t), tile(Q, x, t)
        return r, [q[f] - theta * r[f] for f in range(N)]

    def get_h2(x, t):
        r, q = tile(V, x, t), tile(Q, x, t)
        z = [q[f] - theta * r[f] for f in range(N)]
        return z, z

    def get_h3(x, t):
        r, q = tile(V, x, t), tile(Q, x, t)
        s = [S[f, x, pl.ds(8 * t, 8)] for f in range(N)]
        z = [q[f] - theta * r[f] for f in range(N)]
        return z, [s[f] - theta * q[f] for f in range(N)]

    parts2 = [zero] * N
    parts2 = spread(parts2, gram_loop(get_h1), 0)
    parts2 = spread(parts2, gram_loop(get_h2), 8)
    parts2 = spread(parts2, gram_loop(get_h3), 16)
    value = fold(parts2)
    for axis in axes:
        reduce_start(1, axis, value)
        value = reduce_finish(1, axis)

    h1, h2, h3 = value, shift(value, -8), shift(value, -16)
    g1 = theta * own_gram + h1
    solved = eliminate(pack_lanes([g1, own_gram, h1]))
    alpha, rest = shift(solved, -8), shift(solved, -16)
    h1a, h2a = product(h1, alpha), product(h2, alpha)
    norm_next = product_t(rest, product(own_gram, rest) - h1a) + product_t(
        alpha, h2a - product(h1, rest)
    )
    beta = shift(eliminate(pack_lanes([own_gram, norm_next])), -8)
    mix = rest + beta
    cross = h2 + theta * h1
    curve = product_t(mix, product(g1, mix) - product(cross, alpha)) + product_t(
        alpha, product(h3, alpha) - product(cross, mix)
    )
    alpha2 = shift(eliminate(pack_lanes([curve, norm_next])), -8)
    second = product(alpha, alpha2)
    main = alpha + product(mix, alpha2) + theta * second
    c_out[pl.ds(0, 8)] = main
    c_out[pl.ds(8, 8)] = second

    store_q.wait()
    store_s.wait()
    for d in flat:
        sent_if(d, field_part(d, V, send1, recv1))
        sent_if(d, field_part(d, Q, send2, recv2))
    for d in flat_w:
        sent_if(d, weight_part(d))
    for d in cols:
        sent_if(d, column_part(d, True))
        sent_if(d, column_part(d, False))
    for which in range(2):
        for axis in axes:
            for copy in reduce_copies(which, axis):
                copy.wait_send()


def finish_kernel(c_ref, r_ref, q_ref, s_ref, x_out, r_out):
    planes = r_ref.shape[1]
    for j in range(N):
        main = [c_ref[i, j] for i in range(N)]
        second = [c_ref[N + i, j] for i in range(N)]

        def body(p, carry):
            for t in range(4):
                at = pl.ds(8 * t, 8)
                r = [r_ref[f, p, at] for f in range(N)]
                q = [q_ref[f, p, at] for f in range(N)]
                s = [s_ref[f, p, at] for f in range(N)]
                x = main[0] * r[0] - second[0] * q[0]
                res = second[0] * s[0] - main[0] * q[0]
                for i in range(1, N):
                    x = x + (main[i] * r[i] - second[i] * q[i])
                    res = res + (second[i] * s[i] - main[i] * q[i])
                x_out[j, p, at] = x
                r_out[j, p, at] = r[j] + res
            return carry

        lax.fori_loop(0, planes, body, 0)


def shards(sizes, rhs, stencil):
    nx, ny, nz = sizes
    block = rhs.shape
    anyspace = pl.BlockSpec(memory_space=pl.ANY)
    q, s, coef = pl.pallas_call(
        functools.partial(kernel, sizes),
        out_shape=(
            jax.ShapeDtypeStruct(block, F32),
            jax.ShapeDtypeStruct(block, F32),
            jax.ShapeDtypeStruct((16, 128), F32),
        ),
        in_specs=[anyspace, anyspace],
        out_specs=(anyspace, anyspace, pl.BlockSpec(memory_space=pltpu.VMEM)),
        scratch_shapes=[
            pltpu.VMEM((8, 18, 48, 128), F32),
            pltpu.VMEM((8, 18, 48, 128), F32),
            pltpu.VMEM((14, 17, 48, 128), F32),
            pltpu.VMEM((27, 16, 32, 128), F32),
            pltpu.VMEM((9, 16, 32, 128), F32),
            pltpu.VMEM((16, 32, 128), F32),
            pltpu.VMEM((2, 2, 32, 128), F32),
            pltpu.VMEM((2, 2, 4, 48, 128), F32),
            pltpu.VMEM((2, 32, 128), F32),
            pltpu.VMEM((2, 4, 48, 128), F32),
            pltpu.VMEM((18, 48, 128), F32),
            pltpu.VMEM((17, 48, 128), F32),
            pltpu.VMEM((8, 16, 32, 128), F32),
            pltpu.VMEM((2, 3, 8, 128), F32),
            pltpu.VMEM((2, nx + ny + nz, 8, 128), F32),
            pltpu.SemaphoreType.DMA((2,)),
            pltpu.SemaphoreType.DMA((2,)),
            pltpu.SemaphoreType.DMA((31,)),
            pltpu.SemaphoreType.DMA((31,)),
            pltpu.SemaphoreType.DMA((26,)),
            pltpu.SemaphoreType.DMA((26,)),
            pltpu.SemaphoreType.DMA((2, nx + ny + nz)),
            pltpu.SemaphoreType.DMA((2, nx + ny + nz)),
        ],
        compiler_params=pltpu.CompilerParams(
            collective_id=0, has_side_effects=True, vmem_limit_bytes=50 * 2**20
        ),
        name="operator",
    )(rhs, stencil)
    planes = 2
    spec = pl.BlockSpec((8, planes, 32, 128), lambda i: (0, i, 0, 0))
    return pl.pallas_call(
        finish_kernel,
        grid=(block[1] // planes,),
        out_shape=(jax.ShapeDtypeStruct(block, F32), jax.ShapeDtypeStruct(block, F32)),
        in_specs=[pl.BlockSpec(memory_space=pltpu.SMEM), spec, spec, spec],
        out_specs=(spec, spec),
        name="finish",
    )(coef[:, :8], rhs, q, s)


def solution(mesh):
    sizes = tuple(mesh.shape[n] for n in ("gx", "gy", "gz"))
    placed = P(None, "gx", "gy", "gz")
    return jax.shard_map(
        functools.partial(shards, sizes),
        mesh=mesh,
        in_specs=(placed, placed),
        out_specs=(placed, placed),
        check_vma=False,
    )
```

```python
import functools

import jax
import jax.numpy as jnp
from jax import lax
from jax.experimental import pallas as pl
from jax.experimental.pallas import tpu as pltpu
from jax.sharding import PartitionSpec as P

F32 = jnp.float32
N = 8
FORWARD = [
    (a, b, c) for a in (-1, 0, 1) for b in (-1, 0, 1) for c in (-1, 0, 1) if (a, b, c) > (0, 0, 0)
]
INDEX = {o: k + 1 for k, o in enumerate(FORWARD)}
PLANE = [(a, b) for a in (-1, 0, 1) for b in (-1, 0, 1)]
SLOTS = [(0, 0), (0, 1), (1, -1), (1, 0), (1, 1)]
LOW = [INDEX[(a, b, 1)] for a, b in SLOTS]
UP = [INDEX[(a, b, -1)] if (a, b) != (0, 0) else INDEX[(0, 0, 1)] for a, b in SLOTS]
DIRS = [
    (a, b, c) for a in (-1, 0, 1) for b in (-1, 0, 1) for c in (-1, 0, 1) if (a, b, c) != (0, 0, 0)
]
WRANGE = {(1, 0): (5, 9), (1, 1): (11, 3), (1, -1): (5, 3), (0, 1): (2, 12), (0, -1): (5, 3)}
WDIRS = list(WRANGE)
PAIRS = [(i, j) for i in range(N) for j in range(i, N)]
TOP = 8


def lanes():
    return lax.broadcasted_iota(jnp.int32, (8, 128), 1)


def rows():
    return lax.broadcasted_iota(jnp.int32, (8, 128), 0)


def splat_row(m, k):
    return jnp.broadcast_to(m[k : k + 1, :], (8, 128))


def splat_col(m, k):
    return jnp.broadcast_to(m[:, k : k + 1], (8, 128))


def row_sum(m):
    return jnp.broadcast_to(jnp.sum(m, axis=1, keepdims=True), (8, 128))


def shift(m, amount):
    amount = amount % 128
    return pltpu.roll(m, amount, 1) if amount else m


def product(a, b):
    total = splat_col(a, 0) * splat_row(b, 0)
    for k in range(1, N):
        total = total + splat_col(a, k) * splat_row(b, k)
    return total


def product_t(a, b):
    same = lanes() == rows()
    total = None
    for k in range(N):
        column = row_sum(jnp.where(same, splat_row(a, k), 0.0))
        term = column * splat_row(b, k)
        total = term if total is None else total + term
    return total


def eliminate(m):
    row_id = rows()
    for k in range(N):
        pivot = splat_row(m, k)
        scaled = pivot / splat_col(pivot, k)
        m = jnp.where(row_id == k, scaled, m - splat_col(m, k) * scaled)
    return m


def pack_lanes(parts):
    lane = lanes()
    total = None
    for slot, part in enumerate(parts):
        here = (lane >= 8 * slot) & (lane < 8 * slot + 8)
        term = jnp.where(here, shift(part, 8 * slot), 0.0)
        total = term if total is None else total + term
    return total


def kernel(
    sizes,
    x_ref,
    w_ref,
    X1,
    R1,
    D2,
    A2,
    T,
    V,
    Q,
    S,
    TA,
    W,
    PX,
    WW,
    WE,
    R,
    PP,
    LPP,
    PQ,
    LPQ,
    G,
    GW,
    ARS,
    ARL,
    load_sem,
    send1,
    recv1,
    send2,
    recv2,
    ar_send,
    ar_recv,
):
    names = ("gx", "gy", "gz")
    nx, ny, nz = sizes
    me = tuple(lax.axis_index(n) for n in names)

    def exists(d):
        cond = None
        for pos, step, count in zip(me, d, sizes):
            term = None
            if step > 0:
                term = pos < count - 1
            elif step < 0:
                term = pos > 0
            if term is not None:
                cond = term if cond is None else cond & term
        return cond

    def opposite(d):
        return tuple(-t for t in d)

    def target(d):
        return tuple(pos + step for pos, step in zip(me, d))

    groups = ((1,), (0, 2))
    offsets = (
        [(0, p, 0) for p in range(1, ny)],
        [(p, 0, r) for p in range(nx) for r in range(nz) if p or r],
    )
    own_slot = (me[1], ny + me[0] * nz + me[2])
    slots = ((0, ny), (ny, nx * nz))

    def peer(d):
        return tuple(lax.rem(pos + p, n) if p else pos for pos, p, n in zip(me, d, sizes))

    load_x = pltpu.make_async_copy(x_ref, V.at[:, pl.ds(1, 16), pl.ds(TOP, 32)], load_sem.at[0])
    load_w = pltpu.make_async_copy(w_ref, W.at[:, pl.ds(1, 16), pl.ds(TOP, 32)], load_sem.at[1])
    load_x.start()
    load_w.start()

    zero = jnp.zeros((8, 128), F32)

    def clear_padded(buf, first, last):
        for field in range(buf.shape[0]):
            for plane in (first, last):
                if plane is not None:
                    for t in range(6):
                        buf[field, plane, pl.ds(8 * t, 8)] = zero

        def body(p, carry):
            for field in range(buf.shape[0]):
                buf[field, p, pl.ds(0, 8)] = zero
                buf[field, p, pl.ds(40, 8)] = zero
            return carry

        lax.fori_loop(1, 17, body, 0)

    clear_padded(V, 0, 17)
    clear_padded(Q, 0, 17)
    clear_padded(W, 0, None)

    def clear_landing(i, carry):
        for t in range(6):
            for s in range(2):
                for k in range(2):
                    LPP[s, k, i, pl.ds(8 * t, 8)] = zero
                LPQ[s, i, pl.ds(8 * t, 8)] = zero
        return carry

    lax.fori_loop(0, 4, clear_landing, 0)

    barrier = pltpu.get_barrier_semaphore()
    for d in DIRS:

        @pl.when(exists(d))
        def _():
            pl.semaphore_signal(
                barrier, inc=1, device_id=target(d), device_id_type=pl.DeviceIdType.MESH
            )

    for step in range(2):
        for d in offsets[step]:
            pl.semaphore_signal(
                barrier, inc=1, device_id=peer(d), device_id_type=pl.DeviceIdType.MESH
            )
    span = []
    for pos, count in zip(me, sizes):
        span.append(1 + (pos > 0).astype(jnp.int32) + (pos < count - 1).astype(jnp.int32))
    pl.semaphore_wait(
        barrier, span[0] * span[1] * span[2] - 1 + (ny - 1) + (nx * nz - 1)
    )

    def along(step, whole, plus, minus):
        if step == 0:
            return (pl.ds(*whole), pl.ds(*whole))
        src, dst = plus if step > 0 else minus
        return (pl.ds(src, 1), pl.ds(dst, 1))

    def field_part(d, buf, sends, recvs):
        i = DIRS.index(d)
        xs, xd = along(d[0], (1, 16), (16, 0), (1, 17))
        ys, yd = along(d[1], (TOP, 32), (TOP + 31, TOP - 1), (TOP, TOP + 32))
        return pltpu.make_async_remote_copy(
            src_ref=buf.at[:, xs, ys],
            dst_ref=buf.at[:, xd, yd],
            send_sem=sends.at[i],
            recv_sem=recvs.at[i],
            device_id=target(d),
            device_id_type=pl.DeviceIdType.MESH,
        )

    def weight_part(d):
        i = 26 + WDIRS.index((d[0], d[1]))
        k0, kn = WRANGE[(d[0], d[1])]
        xs, xd = along(d[0], (1, 16), (16, 0), (1, 17))
        ys, yd = along(d[1], (TOP, 32), (TOP + 31, TOP - 1), (TOP, TOP + 32))
        return pltpu.make_async_remote_copy(
            src_ref=W.at[pl.ds(k0, kn), xs, ys],
            dst_ref=W.at[pl.ds(k0, kn), xd, yd],
            send_sem=send1.at[i],
            recv_sem=recv1.at[i],
            device_id=target(d),
            device_id_type=pl.DeviceIdType.MESH,
        )

    def column_part(d, both):
        i = DIRS.index(d)
        side = 0 if d[2] > 0 else 1
        if d[0] == 0:
            gs, gd = pl.ds(0, 2), pl.ds(1, 2)
        elif d[0] > 0:
            gs, gd = pl.ds(1, 1), pl.ds(0, 1)
        else:
            gs, gd = pl.ds(0, 1), pl.ds(3, 1)
        if d[1] == 0:
            ys, yd = pl.ds(0, 32), pl.ds(TOP, 32)
        elif d[1] > 0:
            ys, yd = pl.ds(31, 1), pl.ds(TOP - 1, 1)
        else:
            ys, yd = pl.ds(0, 1), pl.ds(TOP + 32, 1)
        src = PP.at[:, gs, ys] if both else PQ.at[gs, ys]
        dst = LPP.at[side, :, gd, yd] if both else LPQ.at[side, gd, yd]
        return pltpu.make_async_remote_copy(
            src_ref=src,
            dst_ref=dst,
            send_sem=(send1 if both else send2).at[i],
            recv_sem=(recv1 if both else recv2).at[i],
            device_id=target(d),
            device_id_type=pl.DeviceIdType.MESH,
        )

    def start_if(d, copy):
        @pl.when(exists(d))
        def _():
            copy.start()

    def recv_if(d, copy):
        @pl.when(exists(opposite(d)))
        def _():
            copy.wait_recv()

    def sent_if(d, copy):
        @pl.when(exists(d))
        def _():
            copy.wait_send()

    flat = sorted((d for d in DIRS if d[2] == 0), key=lambda d: abs(d[1]))
    flat_w = [(a, b, 0) for a, b in WDIRS]
    cols = [d for d in DIRS if d[2] != 0]

    lane = lanes()
    odd = lax.rem(lane, 2) == 1
    first = lane == 0
    last = lane == 127
    half = lane // 2

    def gather_columns(fields):
        total = zero
        for slot, v in enumerate(fields):
            total = jnp.where(half == slot, shift(v, 2 * slot + 1), total)
        return total

    def merge_columns(dst):
        def body(xg, carry):
            for t in range(4):
                at = pl.ds(8 * t, 8)
                parts = [
                    jnp.where(lane // 16 == xm, shift(PX[xg * 8 + xm, at], 16 * xm), 0.0)
                    for xm in range(8)
                ]
                while len(parts) > 1:
                    parts = [a + b for a, b in zip(parts[::2], parts[1::2])]
                dst(xg, at, parts[0])
            return carry

        lax.fori_loop(0, 2, body, 0)

    def pack(dst, group):
        def body(x, carry):
            for t in range(4):
                PX[x, pl.ds(8 * t, 8)] = gather_columns(
                    group(x + 1, pl.ds(TOP + 8 * t, 8))
                )
            return carry

        lax.fori_loop(0, 16, body, 0)
        merge_columns(dst)

    def put_weights(xg, at, total):
        PP[1, xg, at] = total

    def weight_group(p, at):
        return [jnp.where(first, W[UP[j], p, at], W[LOW[j], p, at]) for j in range(5)]

    def unpack(get, dst, planes):
        def body(t, carry):
            r0 = pl.multiple_of(8 * t, 8)
            merged = {}
            for xi in planes:
                if xi == 0:
                    g, off = 0, 112
                elif xi == 17:
                    g, off = 3, 0
                else:
                    g, off = 1 + (xi - 1) // 8, 16 * ((xi - 1) % 8)
                if g not in merged:
                    merged[g] = jnp.where(odd, get(1, g, r0), get(0, g, r0))
                dst[xi, pl.ds(r0, 8)] = shift(merged[g], -off)
            return carry

        lax.fori_loop(0, 6, body, 0)

    flat_y = [d for d in flat if d[0] == 0]
    flat_x = [d for d in flat if d[0] != 0]
    flat_wy = [d for d in flat_w if d[0] == 0]
    flat_wx = [d for d in flat_w if d[0] != 0]
    cols_y = [d for d in cols if d[0] == 0]
    cols_x = [d for d in cols if d[0] != 0]

    load_x.wait()
    for d in flat_y + flat_x:
        start_if(d, field_part(d, V, send1, recv1))

    def put_pp(xg, at, total):
        PP[0, xg, at] = total

    pack(put_pp, lambda p, at: [V[f, p, at] for f in range(N)])
    load_w.wait()
    for d in flat_wy:
        start_if(d, weight_part(d))
    pack(put_weights, weight_group)
    for d in cols_y + cols_x:
        start_if(d, column_part(d, True))
    for d in flat_wx:
        start_if(d, weight_part(d))

    def m_of(a, b):
        return 3 * (a + 1) + (b + 1)

    def spread_columns(v, even_from, odd_from):
        return jnp.take_along_axis(v, jnp.where(odd, odd_from, even_from), axis=1)

    def prepare_own(x, carry):
        for t in range(4):
            out = pl.ds(8 * t, 8)
            own = [W[k, x + 1, pl.ds(TOP + 8 * t, 8)] for k in range(14)]
            diag = (own[0] + own[1]) + (own[2] + own[3])
            for k in range(4, 14, 2):
                diag = diag + (own[k] + own[k + 1])
            WW[0, x, out] = diag
            for j, (a, b) in enumerate(SLOTS):
                WW[1 + j, x, out] = shift(own[LOW[j]], 1)
                if j:
                    WW[5 + j, x, out] = shift(own[UP[j]], 127)
                    WE[m_of(a, b), x, out] = spread_columns(
                        jnp.where(first, own[UP[j]], own[LOW[j]]), 0, 127
                    )
        return carry

    def prepare(x, carry):
        for t in range(4):
            r0 = TOP + 8 * t

            def w_at(k, a=0, b=0):
                return W[k, x + 1 + a, pl.ds(r0 + b, 8)]

            out = pl.ds(8 * t, 8)
            diag = WW[0, x, out]
            ahead = zero
            behind = w_at(LOW[0])
            own = spread_columns(
                jnp.where(last, behind, GW[x + 1, pl.ds(r0, 8)]), 0, 127
            )
            WE[m_of(0, 0), x, out] = own
            edge = jnp.where(odd, 0.0, own)
            for j, (a, b) in enumerate(SLOTS):
                if j == 0:
                    continue
                back = spread_columns(GW[x + 1 - a, pl.ds(r0 - b, 8)], 2 * j, 2 * j + 1)
                WE[m_of(-a, -b), x, out] = back
                edge = edge + back
                diag = diag + w_at(INDEX[(a, b, 0)], -a, -b)
                ahead = ahead + w_at(UP[j], -a, -b)
                behind = behind + w_at(LOW[j], -a, -b)
            diag = diag + jnp.where(last, edge, shift(ahead, 127))
            diag = diag + jnp.where(first, edge, shift(behind, 1))
            WW[0, x, out] = diag
        return carry

    lax.fori_loop(0, 16, prepare_own, 0)

    def gram_loop(get):
        sums = []
        for lo, hi in ((0, 3), (3, N)):
            pairs = [(i, j) for i, j in PAIRS if lo <= i < hi]

            def body(x, acc):
                acc = list(acc)
                for t in range(4):
                    left, right = get(x, t, range(lo, hi), range(lo, N))
                    for n, (i, j) in enumerate(pairs):
                        acc[n] = acc[n] + left[i] * right[j]
                return tuple(acc)

            sums += list(lax.fori_loop(0, 16, body, tuple(zero for _ in pairs)))
        return sums

    def spread(parts, acc, offset):
        for n, (i, j) in enumerate(PAIRS):
            total = row_sum(acc[n])
            parts[i] = jnp.where(lane == offset + j, total, parts[i])
            if i != j:
                parts[j] = jnp.where(lane == offset + i, total, parts[j])
        return parts

    def fold(parts):
        result = zero
        for i in range(N):
            total = jnp.broadcast_to(jnp.sum(parts[i], axis=0, keepdims=True), (8, 128))
            result = jnp.where(rows() == i, total, result)
        return result

    def row(buf, f, x, t):
        return buf[f, x + 1, pl.ds(TOP + 8 * t, 8)]

    def get_rr(x, t, left, right):
        v = {f: row(V, f, x, t) for f in right}
        return v, v

    parts1 = spread([zero] * N, gram_loop(get_rr), 0)

    for d in flat_y:
        recv_if(d, field_part(d, V, send1, recv1))
    for d in flat_wy:
        recv_if(d, weight_part(d))
    for d in cols_y:
        recv_if(d, column_part(d, True))

    def get_lpp(k):
        return lambda s, g, r0: LPP[s, k, g, pl.ds(r0, 8)]

    def get_lpq(s, g, r0):
        return LPQ[s, g, pl.ds(r0, 8)]

    unpack(get_lpp(0), G, range(1, 17))
    unpack(get_lpp(1), GW, range(1, 17))

    def edges(x, carry):
        for t in range(4):
            total = zero
            for a, b in PLANE:
                total = total + WE[m_of(a, b), x, pl.ds(8 * t, 8)] * G[
                    x + 1 + a, pl.ds(TOP + 8 * t + b, 8)
                ]
            R[x, pl.ds(8 * t, 8)] = total
        return carry

    def coupling(x, t, a, b, c):
        j = SLOTS.index((a, b)) if (a, b) in SLOTS else SLOTS.index((-a, -b))
        here = pl.ds(8 * t, 8)
        away = W.at[:, x + 1 + a, pl.ds(TOP + 8 * t + b, 8)]
        ahead = (a, b) in SLOTS
        if c == 0:
            if (a, b) == (0, 0):
                return WW[0, x, here]
            if ahead:
                return W[INDEX[(a, b, 0)], x + 1, pl.ds(TOP + 8 * t, 8)]
            return away[INDEX[(-a, -b, 0)]]
        if c == 1:
            return WW[1 + j, x, here] if ahead else away[UP[j]]
        if ahead and j:
            return WW[5 + j, x, here]
        return away[LOW[j]]

    def operate(src, put, pack_too=False):
        def body(x, carry):
            for t in range(4):
                weights = [
                    [coupling(x, t, a, b, c) for a, b in PLANE] for c in (0, 1, -1)
                ]
                halo = R[x, pl.ds(8 * t, 8)]
                columns = zero
                for f in range(N):
                    sums = [None, None, None]
                    for m, (a, b) in enumerate(PLANE):
                        v = src[f, x + 1 + a, pl.ds(TOP + 8 * t + b, 8)]
                        if (a, b) == (0, 0):
                            centre = weights[0][m] * v
                        for c in range(3):
                            if c == 0 and (a, b) == (0, 0):
                                continue
                            term = weights[c][m] * v
                            sums[c] = term if sums[c] is None else sums[c] + term
                    side = shift(halo, -(2 * f + 1))
                    total = centre - sums[0]
                    total = total - shift(jnp.where(first, side, sums[1]), 127)
                    total = total - shift(jnp.where(last, side, sums[2]), 1)
                    put(f, x, t, total)
                    if pack_too:
                        columns = jnp.where(half == f, shift(total, 2 * f + 1), columns)
                if pack_too:
                    PX[x, pl.ds(8 * t, 8)] = columns
            return carry

        return body

    def ends(body):
        return lambda i, carry: body(15 * i, carry)

    def put_q(f, x, t, value):
        Q[f, x + 1, pl.ds(TOP + 8 * t, 8)] = value

    def put_s(f, x, t, value):
        S[f, x, pl.ds(8 * t, 8)] = value

    lax.fori_loop(1, 16, prepare, 0)
    lax.fori_loop(1, 15, edges, 0)
    lax.fori_loop(1, 15, operate(V, put_q, True), 0)
    for d in flat_x:
        recv_if(d, field_part(d, V, send1, recv1))
    for d in flat_wx:
        recv_if(d, weight_part(d))
    for d in cols_x:
        recv_if(d, column_part(d, True))
    unpack(get_lpp(0), G, (0, 17))
    unpack(get_lpp(1), GW, (0,))
    prepare(0, 0)
    lax.fori_loop(0, 2, ends(edges), 0)
    lax.fori_loop(0, 2, ends(operate(V, put_q, True)), 0)

    for d in flat_y + flat_x:
        start_if(d, field_part(d, Q, send2, recv2))

    def put_pq(xg, at, total):
        PQ[xg, at] = total

    merge_columns(put_pq)
    for d in cols_y + cols_x:
        start_if(d, column_part(d, False))

    def reduce_copies(which, step):
        copies = []
        for i, d in enumerate(offsets[step]):
            i = slots[step][0] + i
            copies.append(
                pltpu.make_async_remote_copy(
                    src_ref=ARS.at[which, step],
                    dst_ref=ARL.at[which, own_slot[step]],
                    send_sem=ar_send.at[which, i],
                    recv_sem=ar_recv.at[which, i],
                    device_id=peer(d),
                    device_id_type=pl.DeviceIdType.MESH,
                )
            )
        return copies

    def reduce_start(which, step, value):
        ARS[which, step] = value
        ARL[which, own_slot[step]] = value
        for copy in reduce_copies(which, step):
            copy.start()

    def reduce_finish(which, step):
        for copy in reduce_copies(which, step):
            copy.wait_recv()
        lo, count = slots[step]
        parts = [ARL[which, lo + i] for i in range(count)]
        while len(parts) > 1:
            parts = [a + b for a, b in zip(parts[::2], parts[1::2])]
        return parts[0]

    def get_rq(x, t, left, right):
        return (
            {f: row(V, f, x, t) for f in left},
            {f: row(Q, f, x, t) for f in right},
        )

    def get_qq(x, t, left, right):
        q = {f: row(Q, f, x, t) for f in right}
        return q, q

    parts1 = spread(parts1, gram_loop(get_rq), 8)
    parts1 = spread(parts1, gram_loop(get_qq), 16)
    reduce_start(0, 0, fold(parts1))

    for d in flat_y:
        recv_if(d, field_part(d, Q, send2, recv2))
    for d in cols_y:
        recv_if(d, column_part(d, False))
    unpack(get_lpq, G, range(1, 17))
    lax.fori_loop(1, 15, edges, 0)
    lax.fori_loop(1, 5, operate(Q, put_s), 0)
    reduce_start(0, 1, reduce_finish(0, 0))
    lax.fori_loop(5, 15, operate(Q, put_s), 0)
    for d in flat_x:
        recv_if(d, field_part(d, Q, send2, recv2))
    for d in cols_x:
        recv_if(d, column_part(d, False))
    unpack(get_lpq, G, (0, 17))
    lax.fori_loop(0, 2, ends(edges), 0)
    lax.fori_loop(0, 2, ends(operate(Q, put_s)), 0)
    sum1 = reduce_finish(0, 1)

    def trace(m):
        total = row_sum(jnp.where(lane == rows(), m, 0.0))
        return jnp.broadcast_to(jnp.sum(total, axis=0, keepdims=True), (8, 128))

    small = lane < 8
    own_gram = jnp.where(small, sum1, 0.0)
    g1 = jnp.where(small, shift(sum1, -8), 0.0)
    g2 = shift(sum1, -16)
    theta = trace(g1) / trace(own_gram)
    h1 = g1 - theta * own_gram

    def moved(f, x, t):
        return row(Q, f, x, t) - theta * row(V, f, x, t)

    def get_h2(x, t, left, right):
        z = {f: moved(f, x, t) for f in right}
        return z, z

    def get_zs(x, t, left, right):
        return (
            {f: moved(f, x, t) for f in left},
            {f: S[f, x, pl.ds(8 * t, 8)] for f in right},
        )

    parts2 = [zero] * N
    parts2 = spread(parts2, gram_loop(get_h2), 0)
    parts2 = spread(parts2, gram_loop(get_zs), 8)
    reduce_start(1, 0, fold(parts2))

    unit = jnp.where(lane == rows(), 1.0, 0.0)
    solved = eliminate(pack_lanes([g1, own_gram, h1]))
    inverse = shift(eliminate(pack_lanes([own_gram, unit])), -8)
    alpha, rest = shift(solved, -8), shift(solved, -16)
    beta = own_gram - product(g1, alpha) + product_t(alpha, product(g2, alpha) - g1)
    beta = product(inverse, beta)
    mix = rest + beta
    early = product(own_gram, rest) - product(h1, alpha)
    early = product_t(rest, early) - product_t(alpha, product(h1, rest))

    def put_table(dst, base, m):
        for i in range(N):
            line = splat_row(m, i)
            for j in range(N):
                dst[base + N * j + i] = splat_col(line, j)

    put_table(TA, 0, alpha)
    put_table(TA, 64, unit + beta)

    def second_body(j, carry):
        a = [TA[N * j + i] for i in range(N)]
        b = [TA[64 + N * j + i] for i in range(N)]

        def body(x, carry):
            for t in range(4):
                at = pl.ds(8 * t, 8)
                r = [row(V, f, x, t) for f in range(N)]
                q = [row(Q, f, x, t) for f in range(N)]
                s = [S[f, x, at] for f in range(N)]

                def comb(c, v):
                    total = c[0] * v[0]
                    for i in range(1, N):
                        total = total + c[i] * v[i]
                    return total

                aq = comb(a, q)
                X1[j, x, at] = comb(a, r)
                R1[j, x, at] = row(V, j, x, t) - aq
                D2[j, x, at] = comb(b, r) - aq
                A2[j, x, at] = comb(b, q) - comb(a, s)
            return carry

        lax.fori_loop(0, 16, body, 0)
        return carry

    lax.fori_loop(0, 2, second_body, 0)
    reduce_start(1, 1, reduce_finish(1, 0))
    lax.fori_loop(2, N, second_body, 0)
    sum2 = reduce_finish(1, 1)

    h2, zs = sum2, shift(sum2, -8)
    norm_next = early + product_t(alpha, product(h2, alpha))
    cross = h2 + theta * h1
    h3 = zs - theta * cross
    curve = product_t(mix, product(g1, mix) - product(cross, alpha)) + product_t(
        alpha, product(h3, alpha) - product(cross, mix)
    )
    alpha2 = shift(eliminate(pack_lanes([curve, norm_next])), -8)
    put_table(T, 0, alpha2)

    for d in flat:
        sent_if(d, field_part(d, V, send1, recv1))
        sent_if(d, field_part(d, Q, send2, recv2))
    for d in flat_w:
        sent_if(d, weight_part(d))
    for d in cols:
        sent_if(d, column_part(d, True))
        sent_if(d, column_part(d, False))
    for which in range(2):
        for step in range(2):
            for copy in reduce_copies(which, step):
                copy.wait_send()


def finish_kernel(X1, R1, D2, A2, T, x_out, r_out, X, Y, sems):
    def store(j):
        return [
            pltpu.make_async_copy(buf.at[j], out.at[j], sems.at[k, j])
            for k, (buf, out) in enumerate(((X, x_out), (Y, r_out)))
        ]

    for j in range(N):
        a = [T[N * j + i] for i in range(N)]

        def body(p, carry):
            for t in range(4):
                at = pl.ds(8 * t, 8)
                x = X1[j, p, at]
                res = R1[j, p, at]
                for i in range(0, N, 2):
                    x = x + (a[i] * D2[i, p, at] + a[i + 1] * D2[i + 1, p, at])
                    res = res - (a[i] * A2[i, p, at] + a[i + 1] * A2[i + 1, p, at])
                X[j, p, at] = x
                Y[j, p, at] = res
            return carry

        lax.fori_loop(0, 16, body, 0)
        for copy in store(j):
            copy.start()
    for j in range(N):
        for copy in store(j):
            copy.wait()


def shards(sizes, rhs, stencil):
    nx, ny, nz = sizes
    block = rhs.shape
    anyspace = pl.BlockSpec(memory_space=pl.ANY)
    local = pl.BlockSpec(memory_space=pltpu.VMEM)
    hbm = pl.BlockSpec(memory_space=pltpu.HBM)
    field = jax.ShapeDtypeStruct(block, F32)
    kept = pl.pallas_call(
        functools.partial(kernel, sizes),
        out_shape=(field,) * 4 + (jax.ShapeDtypeStruct((64, 8, 128), F32),),
        in_specs=[hbm, hbm],
        out_specs=(local,) * 5,
        scratch_shapes=[
            pltpu.VMEM((8, 18, 48, 128), F32),
            pltpu.VMEM((8, 18, 48, 128), F32),
            pltpu.VMEM(block, F32),
            pltpu.VMEM((128, 8, 128), F32),
            pltpu.VMEM((14, 17, 48, 128), F32),
            pltpu.VMEM((16, 32, 128), F32),
            pltpu.VMEM((10, 16, 32, 128), F32),
            pltpu.VMEM((9, 16, 32, 128), F32),
            pltpu.VMEM((16, 32, 128), F32),
            pltpu.VMEM((2, 2, 32, 128), F32),
            pltpu.VMEM((2, 2, 4, 48, 128), F32),
            pltpu.VMEM((2, 32, 128), F32),
            pltpu.VMEM((2, 4, 48, 128), F32),
            pltpu.VMEM((18, 48, 128), F32),
            pltpu.VMEM((17, 48, 128), F32),
            pltpu.VMEM((2, 2, 8, 128), F32),
            pltpu.VMEM((2, ny + nx * nz, 8, 128), F32),
            pltpu.SemaphoreType.DMA((2,)),
            pltpu.SemaphoreType.DMA((31,)),
            pltpu.SemaphoreType.DMA((31,)),
            pltpu.SemaphoreType.DMA((26,)),
            pltpu.SemaphoreType.DMA((26,)),
            pltpu.SemaphoreType.DMA((2, ny + nx * nz)),
            pltpu.SemaphoreType.DMA((2, ny + nx * nz)),
        ],
        compiler_params=pltpu.CompilerParams(
            collective_id=0, has_side_effects=True, vmem_limit_bytes=44 * 2**20
        ),
        name="operator",
    )(rhs, stencil)
    return pl.pallas_call(
        finish_kernel,
        out_shape=(jax.ShapeDtypeStruct(block, F32), jax.ShapeDtypeStruct(block, F32)),
        in_specs=[local] * 5,
        out_specs=(anyspace, anyspace),
        scratch_shapes=[
            pltpu.VMEM(block, F32),
            pltpu.VMEM(block, F32),
            pltpu.SemaphoreType.DMA((2, N)),
        ],
        compiler_params=pltpu.CompilerParams(vmem_limit_bytes=24 * 2**20),
        name="finish",
    )(*kept)


def solution(mesh):
    sizes = tuple(mesh.shape[n] for n in ("gx", "gy", "gz"))
    placed = P(None, "gx", "gy", "gz")
    return jax.shard_map(
        functools.partial(shards, sizes),
        mesh=mesh,
        in_specs=(placed, placed),
        out_specs=(placed, placed),
        check_vma=False,
    )
```

```python
import functools

import jax
import jax.numpy as jnp
from jax import lax
from jax.experimental import pallas as pl
from jax.experimental.pallas import tpu as pltpu
from jax.sharding import PartitionSpec as P

F32 = jnp.float32
N = 8
FORWARD = [
    (a, b, c) for a in (-1, 0, 1) for b in (-1, 0, 1) for c in (-1, 0, 1) if (a, b, c) > (0, 0, 0)
]
INDEX = {o: k + 1 for k, o in enumerate(FORWARD)}
PLANE = [(a, b) for a in (-1, 0, 1) for b in (-1, 0, 1)]
SLOTS = [(0, 0), (0, 1), (1, -1), (1, 0), (1, 1)]
LOW = [INDEX[(a, b, 1)] for a, b in SLOTS]
UP = [INDEX[(a, b, -1)] if (a, b) != (0, 0) else INDEX[(0, 0, 1)] for a, b in SLOTS]
DIRS = [
    (a, b, c) for a in (-1, 0, 1) for b in (-1, 0, 1) for c in (-1, 0, 1) if (a, b, c) != (0, 0, 0)
]
WRANGE = {(1, 0): (5, 9), (1, 1): (11, 3), (1, -1): (5, 3), (0, 1): (2, 12), (0, -1): (5, 3)}
WDIRS = list(WRANGE)
PAIRS = [(i, j) for i in range(N) for j in range(i, N)]
TOP = 8


def lanes():
    return lax.broadcasted_iota(jnp.int32, (8, 128), 1)


def rows():
    return lax.broadcasted_iota(jnp.int32, (8, 128), 0)


def splat_row(m, k):
    return jnp.broadcast_to(m[k : k + 1, :], (8, 128))


def splat_col(m, k):
    return jnp.broadcast_to(m[:, k : k + 1], (8, 128))


def row_sum(m):
    return jnp.broadcast_to(jnp.sum(m, axis=1, keepdims=True), (8, 128))


def shift(m, amount):
    amount = amount % 128
    return pltpu.roll(m, amount, 1) if amount else m


def columns(m, base=0):
    return [splat_col(m, base + k) for k in range(N)]


def columns_t(m):
    same = lanes() == rows()
    return [row_sum(jnp.where(same, splat_row(m, k), 0.0)) for k in range(N)]


def times(cols, m):
    terms = [cols[k] * splat_row(m, k) for k in range(N)]
    while len(terms) > 1:
        terms = [a + b for a, b in zip(terms[::2], terms[1::2])]
    return terms[0]


def solve(cols, rights):
    cols = list(cols)
    row_id = rows()
    for k in range(N):
        here = row_id == k
        inverse = 1.0 / splat_row(cols[k], k)
        factor = cols[k] * inverse

        def step(m):
            line = splat_row(m, k)
            return jnp.where(here, line * inverse, m - factor * line)

        cols = cols[: k + 1] + [step(c) for c in cols[k + 1 :]]
        rights = [step(r) for r in rights]
    return rights


def kernel(
    sizes,
    x_ref,
    w_ref,
    X1,
    R1,
    D2,
    A2,
    T,
    V,
    Q,
    S,
    TA,
    W,
    PX,
    WW,
    WE,
    R,
    PP,
    LPP,
    PQ,
    LPQ,
    G,
    GW,
    ARS,
    ARL,
    load_sem,
    send1,
    recv1,
    send2,
    recv2,
    ar_send,
    ar_recv,
):
    names = ("gx", "gy", "gz")
    nx, ny, nz = sizes
    me = tuple(lax.axis_index(n) for n in names)

    def exists(d):
        cond = None
        for pos, step, count in zip(me, d, sizes):
            term = None
            if step > 0:
                term = pos < count - 1
            elif step < 0:
                term = pos > 0
            if term is not None:
                cond = term if cond is None else cond & term
        return cond

    def opposite(d):
        return tuple(-t for t in d)

    def target(d):
        return tuple(pos + step for pos, step in zip(me, d))

    groups = ((1,), (0, 2))
    offsets = (
        [(0, p, 0) for p in range(1, ny)],
        [(p, 0, r) for p in range(nx) for r in range(nz) if p or r],
    )
    own_slot = (me[1], ny + me[0] * nz + me[2])
    slots = ((0, ny), (ny, nx * nz))

    def peer(d):
        return tuple(lax.rem(pos + p, n) if p else pos for pos, p, n in zip(me, d, sizes))

    load_x = pltpu.make_async_copy(x_ref, V.at[:, pl.ds(1, 16), pl.ds(TOP, 32)], load_sem.at[0])
    load_w = pltpu.make_async_copy(w_ref, W.at[:, pl.ds(1, 16), pl.ds(TOP, 32)], load_sem.at[1])
    load_x.start()
    load_w.start()

    zero = jnp.zeros((8, 128), F32)

    def clear_padded(buf, first, last):
        for field in range(buf.shape[0]):
            for plane in (first, last):
                if plane is not None:
                    for t in range(6):
                        buf[field, plane, pl.ds(8 * t, 8)] = zero

        def body(p, carry):
            for field in range(buf.shape[0]):
                buf[field, p, pl.ds(0, 8)] = zero
                buf[field, p, pl.ds(40, 8)] = zero
            return carry

        lax.fori_loop(1, 17, body, 0)

    clear_padded(V, 0, 17)
    clear_padded(Q, 0, 17)
    clear_padded(W, 0, None)

    def clear_landing(i, carry):
        for t in range(6):
            for s in range(2):
                for k in range(2):
                    LPP[s, k, i, pl.ds(8 * t, 8)] = zero
                LPQ[s, i, pl.ds(8 * t, 8)] = zero
        return carry

    lax.fori_loop(0, 4, clear_landing, 0)

    barrier = pltpu.get_barrier_semaphore()
    for d in DIRS:

        @pl.when(exists(d))
        def _():
            pl.semaphore_signal(
                barrier, inc=1, device_id=target(d), device_id_type=pl.DeviceIdType.MESH
            )

    for step in range(2):
        for d in offsets[step]:
            pl.semaphore_signal(
                barrier, inc=1, device_id=peer(d), device_id_type=pl.DeviceIdType.MESH
            )
    span = []
    for pos, count in zip(me, sizes):
        span.append(1 + (pos > 0).astype(jnp.int32) + (pos < count - 1).astype(jnp.int32))
    def along(step, whole, plus, minus):
        if step == 0:
            return (pl.ds(*whole), pl.ds(*whole))
        src, dst = plus if step > 0 else minus
        return (pl.ds(src, 1), pl.ds(dst, 1))

    def field_part(d, buf, sends, recvs):
        i = DIRS.index(d)
        xs, xd = along(d[0], (1, 16), (16, 0), (1, 17))
        ys, yd = along(d[1], (TOP, 32), (TOP + 31, TOP - 1), (TOP, TOP + 32))
        return pltpu.make_async_remote_copy(
            src_ref=buf.at[:, xs, ys],
            dst_ref=buf.at[:, xd, yd],
            send_sem=sends.at[i],
            recv_sem=recvs.at[i],
            device_id=target(d),
            device_id_type=pl.DeviceIdType.MESH,
        )

    def weight_part(d):
        i = 26 + WDIRS.index((d[0], d[1]))
        k0, kn = WRANGE[(d[0], d[1])]
        xs, xd = along(d[0], (1, 16), (16, 0), (1, 17))
        ys, yd = along(d[1], (TOP, 32), (TOP + 31, TOP - 1), (TOP, TOP + 32))
        return pltpu.make_async_remote_copy(
            src_ref=W.at[pl.ds(k0, kn), xs, ys],
            dst_ref=W.at[pl.ds(k0, kn), xd, yd],
            send_sem=send1.at[i],
            recv_sem=recv1.at[i],
            device_id=target(d),
            device_id_type=pl.DeviceIdType.MESH,
        )

    def column_part(d, both):
        i = DIRS.index(d)
        side = 0 if d[2] > 0 else 1
        if d[0] == 0:
            gs, gd = pl.ds(0, 2), pl.ds(1, 2)
        elif d[0] > 0:
            gs, gd = pl.ds(1, 1), pl.ds(0, 1)
        else:
            gs, gd = pl.ds(0, 1), pl.ds(3, 1)
        if d[1] == 0:
            ys, yd = pl.ds(0, 32), pl.ds(TOP, 32)
        elif d[1] > 0:
            ys, yd = pl.ds(31, 1), pl.ds(TOP - 1, 1)
        else:
            ys, yd = pl.ds(0, 1), pl.ds(TOP + 32, 1)
        src = PP.at[:, gs, ys] if both else PQ.at[gs, ys]
        dst = LPP.at[side, :, gd, yd] if both else LPQ.at[side, gd, yd]
        return pltpu.make_async_remote_copy(
            src_ref=src,
            dst_ref=dst,
            send_sem=(send1 if both else send2).at[i],
            recv_sem=(recv1 if both else recv2).at[i],
            device_id=target(d),
            device_id_type=pl.DeviceIdType.MESH,
        )

    def start_if(d, copy):
        @pl.when(exists(d))
        def _():
            copy.start()

    def recv_if(d, copy):
        @pl.when(exists(opposite(d)))
        def _():
            copy.wait_recv()

    def sent_if(d, copy):
        @pl.when(exists(d))
        def _():
            copy.wait_send()

    flat = sorted((d for d in DIRS if d[2] == 0), key=lambda d: abs(d[1]))
    flat_w = [(a, b, 0) for a, b in WDIRS]
    cols = [d for d in DIRS if d[2] != 0]

    lane = lanes()
    odd = lax.rem(lane, 2) == 1
    first = lane == 0
    last = lane == 127
    half = lane // 2

    def gather_columns(fields):
        total = zero
        for slot, v in enumerate(fields):
            total = jnp.where(half == slot, shift(v, 2 * slot + 1), total)
        return total

    def merge_columns(dst):
        for xg in range(2):
            for t in range(4):
                at = pl.ds(8 * t, 8)
                parts = [
                    jnp.where(lane // 16 == xm, shift(PX[xg * 8 + xm, at], 16 * xm), 0.0)
                    for xm in range(8)
                ]
                while len(parts) > 1:
                    parts = [a + b for a, b in zip(parts[::2], parts[1::2])]
                dst(xg, at, parts[0])

    def pack(dst, group):
        def body(i, carry):
            for k in range(4):
                x = 4 * i + k
                for t in range(4):
                    PX[x, pl.ds(8 * t, 8)] = gather_columns(
                        group(x + 1, pl.ds(TOP + 8 * t, 8))
                    )
            return carry

        lax.fori_loop(0, 4, body, 0)
        merge_columns(dst)

    def put_weights(xg, at, total):
        PP[1, xg, at] = total

    def weight_group(p, at):
        return [jnp.where(first, W[UP[j], p, at], W[LOW[j], p, at]) for j in range(5)]

    def unpack(get, dst, planes):
        for t in range(6):
            r0 = 8 * t
            merged = {}
            for xi in planes:
                if xi == 0:
                    g, off = 0, 112
                elif xi == 17:
                    g, off = 3, 0
                else:
                    g, off = 1 + (xi - 1) // 8, 16 * ((xi - 1) % 8)
                if g not in merged:
                    merged[g] = jnp.where(odd, get(1, g, r0), get(0, g, r0))
                dst[xi, pl.ds(r0, 8)] = shift(merged[g], -off)

    def blocks(body, first_x, count, width):
        def several(i, carry):
            for k in range(width):
                body(first_x + width * i + k, carry)
            return carry

        lax.fori_loop(0, count, several, 0)

    flat_y = [d for d in flat if d[0] == 0]
    flat_x = [d for d in flat if d[0] != 0]
    flat_wy = [d for d in flat_w if d[0] == 0]
    flat_wx = [d for d in flat_w if d[0] != 0]
    cols_y = [d for d in cols if d[0] == 0]
    cols_x = [d for d in cols if d[0] != 0]

    def put_pp(xg, at, total):
        PP[0, xg, at] = total

    load_x.wait()
    pack(put_pp, lambda p, at: [V[f, p, at] for f in range(N)])
    load_w.wait()
    pack(put_weights, weight_group)

    pl.semaphore_wait(
        barrier, span[0] * span[1] * span[2] - 1 + (ny - 1) + (nx * nz - 1)
    )

    for d in flat_y:
        start_if(d, field_part(d, V, send1, recv1))
    for d in flat_wy:
        start_if(d, weight_part(d))
    for d in cols_y:
        start_if(d, column_part(d, True))
    for d in flat_x:
        start_if(d, field_part(d, V, send1, recv1))
    for d in cols_x:
        start_if(d, column_part(d, True))
    for d in flat_wx:
        start_if(d, weight_part(d))

    def m_of(a, b):
        return 3 * (a + 1) + (b + 1)

    def spread_columns(v, even_from, odd_from):
        return jnp.take_along_axis(v, jnp.where(odd, odd_from, even_from), axis=1)

    def prepare_own(x, carry):
        for t in range(4):
            out = pl.ds(8 * t, 8)
            own = [W[k, x + 1, pl.ds(TOP + 8 * t, 8)] for k in range(14)]
            diag = (own[0] + own[1]) + (own[2] + own[3])
            for k in range(4, 14, 2):
                diag = diag + (own[k] + own[k + 1])
            WW[0, x, out] = diag
            for j, (a, b) in enumerate(SLOTS):
                WW[1 + j, x, out] = shift(own[LOW[j]], 1)
                if j:
                    WW[5 + j, x, out] = shift(own[UP[j]], 127)
                    WE[m_of(a, b), x, out] = spread_columns(
                        jnp.where(first, own[UP[j]], own[LOW[j]]), 0, 127
                    )
        return carry

    def prepare(x, carry):
        for t in range(4):
            r0 = TOP + 8 * t

            def w_at(k, a=0, b=0):
                return W[k, x + 1 + a, pl.ds(r0 + b, 8)]

            out = pl.ds(8 * t, 8)
            diag = WW[0, x, out]
            ahead = zero
            behind = w_at(LOW[0])
            own = spread_columns(
                jnp.where(last, behind, GW[x + 1, pl.ds(r0, 8)]), 0, 127
            )
            WE[m_of(0, 0), x, out] = own
            edge = jnp.where(odd, 0.0, own)
            for j, (a, b) in enumerate(SLOTS):
                if j == 0:
                    continue
                back = spread_columns(GW[x + 1 - a, pl.ds(r0 - b, 8)], 2 * j, 2 * j + 1)
                WE[m_of(-a, -b), x, out] = back
                edge = edge + back
                diag = diag + w_at(INDEX[(a, b, 0)], -a, -b)
                ahead = ahead + w_at(UP[j], -a, -b)
                behind = behind + w_at(LOW[j], -a, -b)
            diag = diag + jnp.where(last, edge, shift(ahead, 127))
            diag = diag + jnp.where(first, edge, shift(behind, 1))
            WW[0, x, out] = diag
        return carry

    blocks(prepare_own, 0, 8, 2)

    def gram_loop(get):
        sums = []
        for lo, hi in ((0, 3), (3, N)):
            pairs = [(i, j) for i, j in PAIRS if lo <= i < hi]

            def body(x, acc):
                acc = list(acc)
                for t in range(4):
                    left, right = get(x, t, range(lo, hi), range(lo, N))
                    for n, (i, j) in enumerate(pairs):
                        acc[n] = acc[n] + left[i] * right[j]
                return tuple(acc)

            sums += list(lax.fori_loop(0, 16, body, tuple(zero for _ in pairs)))
        return sums

    def spread(parts, acc, offset):
        for n, (i, j) in enumerate(PAIRS):
            total = row_sum(acc[n])
            parts[i] = jnp.where(lane == offset + j, total, parts[i])
            if i != j:
                parts[j] = jnp.where(lane == offset + i, total, parts[j])
        return parts

    def fold(parts):
        result = zero
        for i in range(N):
            total = jnp.broadcast_to(jnp.sum(parts[i], axis=0, keepdims=True), (8, 128))
            result = jnp.where(rows() == i, total, result)
        return result

    def row(buf, f, x, t):
        return buf[f, x + 1, pl.ds(TOP + 8 * t, 8)]

    def get_rr(x, t, left, right):
        v = {f: row(V, f, x, t) for f in right}
        return v, v

    parts1 = spread([zero] * N, gram_loop(get_rr), 0)

    for d in flat_y:
        recv_if(d, field_part(d, V, send1, recv1))
    for d in flat_wy:
        recv_if(d, weight_part(d))
    for d in cols_y:
        recv_if(d, column_part(d, True))

    def get_lpp(k):
        return lambda s, g, r0: LPP[s, k, g, pl.ds(r0, 8)]

    def get_lpq(s, g, r0):
        return LPQ[s, g, pl.ds(r0, 8)]

    unpack(get_lpp(0), G, range(1, 17))
    unpack(get_lpp(1), GW, range(1, 17))

    def edges(x, carry):
        for t in range(4):
            total = zero
            for a, b in PLANE:
                total = total + WE[m_of(a, b), x, pl.ds(8 * t, 8)] * G[
                    x + 1 + a, pl.ds(TOP + 8 * t + b, 8)
                ]
            R[x, pl.ds(8 * t, 8)] = total
        return carry

    def coupling(x, t, a, b, c):
        j = SLOTS.index((a, b)) if (a, b) in SLOTS else SLOTS.index((-a, -b))
        here = pl.ds(8 * t, 8)
        away = W.at[:, x + 1 + a, pl.ds(TOP + 8 * t + b, 8)]
        ahead = (a, b) in SLOTS
        if c == 0:
            if (a, b) == (0, 0):
                return WW[0, x, here]
            if ahead:
                return W[INDEX[(a, b, 0)], x + 1, pl.ds(TOP + 8 * t, 8)]
            return away[INDEX[(-a, -b, 0)]]
        if c == 1:
            return WW[1 + j, x, here] if ahead else away[UP[j]]
        if ahead and j:
            return WW[5 + j, x, here]
        return away[LOW[j]]

    def operate(src, put):
        def body(x, carry):
            for t in range(4):
                weights = [
                    [coupling(x, t, a, b, c) for a, b in PLANE] for c in (0, 1, -1)
                ]
                halo = R[x, pl.ds(8 * t, 8)]
                for f in range(N):
                    sums = [None, None, None]
                    for m, (a, b) in enumerate(PLANE):
                        v = src[f, x + 1 + a, pl.ds(TOP + 8 * t + b, 8)]
                        if (a, b) == (0, 0):
                            centre = weights[0][m] * v
                        for c in range(3):
                            if c == 0 and (a, b) == (0, 0):
                                continue
                            term = weights[c][m] * v
                            sums[c] = term if sums[c] is None else sums[c] + term
                    side = shift(halo, -(2 * f + 1))
                    total = centre - sums[0]
                    total = total - shift(jnp.where(first, side, sums[1]), 127)
                    total = total - shift(jnp.where(last, side, sums[2]), 1)
                    put(f, x, t, total)
            return carry

        return body

    def ends(body):
        return lambda i, carry: body(15 * i, carry)

    def put_q(f, x, t, value):
        Q[f, x + 1, pl.ds(TOP + 8 * t, 8)] = value

    def put_s(f, x, t, value):
        S[f, x, pl.ds(8 * t, 8)] = value

    blocks(prepare, 1, 5, 3)
    lax.fori_loop(1, 15, edges, 0)
    lax.fori_loop(1, 15, operate(V, put_q), 0)
    for d in flat_x:
        recv_if(d, field_part(d, V, send1, recv1))
    for d in flat_wx:
        recv_if(d, weight_part(d))
    for d in cols_x:
        recv_if(d, column_part(d, True))
    unpack(get_lpp(0), G, (0, 17))
    unpack(get_lpp(1), GW, (0,))
    prepare(0, 0)
    lax.fori_loop(0, 2, ends(edges), 0)
    lax.fori_loop(0, 2, ends(operate(V, put_q)), 0)

    for d in flat_y + flat_x:
        start_if(d, field_part(d, Q, send2, recv2))

    def put_pq(xg, at, total):
        PQ[xg, at] = total

    pack(put_pq, lambda p, at: [Q[f, p, at] for f in range(N)])
    for d in cols_y + cols_x:
        start_if(d, column_part(d, False))

    def reduce_copies(which, step):
        copies = []
        for i, d in enumerate(offsets[step]):
            i = slots[step][0] + i
            copies.append(
                pltpu.make_async_remote_copy(
                    src_ref=ARS.at[which, step],
                    dst_ref=ARL.at[which, own_slot[step]],
                    send_sem=ar_send.at[which, i],
                    recv_sem=ar_recv.at[which, i],
                    device_id=peer(d),
                    device_id_type=pl.DeviceIdType.MESH,
                )
            )
        return copies

    def reduce_start(which, step, value):
        ARS[which, step] = value
        ARL[which, own_slot[step]] = value
        for copy in reduce_copies(which, step):
            copy.start()

    def reduce_finish(which, step):
        for copy in reduce_copies(which, step):
            copy.wait_recv()
        lo, count = slots[step]
        parts = [ARL[which, lo + i] for i in range(count)]
        while len(parts) > 1:
            parts = [a + b for a, b in zip(parts[::2], parts[1::2])]
        return parts[0]

    def get_rq(x, t, left, right):
        return (
            {f: row(V, f, x, t) for f in left},
            {f: row(Q, f, x, t) for f in right},
        )

    def get_qq(x, t, left, right):
        q = {f: row(Q, f, x, t) for f in right}
        return q, q

    parts1 = spread(parts1, gram_loop(get_rq), 8)
    parts1 = spread(parts1, gram_loop(get_qq), 16)
    reduce_start(0, 0, fold(parts1))

    for d in flat_y:
        recv_if(d, field_part(d, Q, send2, recv2))
    for d in cols_y:
        recv_if(d, column_part(d, False))
    unpack(get_lpq, G, range(1, 17))
    lax.fori_loop(1, 15, edges, 0)
    lax.fori_loop(1, 5, operate(Q, put_s), 0)
    reduce_start(0, 1, reduce_finish(0, 0))
    lax.fori_loop(5, 15, operate(Q, put_s), 0)
    for d in flat_x:
        recv_if(d, field_part(d, Q, send2, recv2))
    for d in cols_x:
        recv_if(d, column_part(d, False))
    unpack(get_lpq, G, (0, 17))
    lax.fori_loop(0, 2, ends(edges), 0)
    lax.fori_loop(0, 2, ends(operate(Q, put_s)), 0)
    sum1 = reduce_finish(0, 1)

    def trace(m):
        total = row_sum(jnp.where(lane == rows(), m, 0.0))
        return jnp.broadcast_to(jnp.sum(total, axis=0, keepdims=True), (8, 128))

    small = lane < 8
    own_gram = jnp.where(small, sum1, 0.0)
    g1 = jnp.where(small, shift(sum1, -8), 0.0)
    g2 = shift(sum1, -16)
    theta = trace(g1) / trace(own_gram)
    h1 = g1 - theta * own_gram

    def moved(f, x, t):
        return row(Q, f, x, t) - theta * row(V, f, x, t)

    def get_h2(x, t, left, right):
        z = {f: moved(f, x, t) for f in right}
        return z, z

    def get_zs(x, t, left, right):
        return (
            {f: moved(f, x, t) for f in left},
            {f: S[f, x, pl.ds(8 * t, 8)] for f in right},
        )

    parts2 = [zero] * N
    parts2 = spread(parts2, gram_loop(get_h2), 0)
    parts2 = spread(parts2, gram_loop(get_zs), 8)
    reduce_start(1, 0, fold(parts2))

    unit = jnp.where(lane == rows(), 1.0, 0.0)
    g1_cols, h1_cols = columns(g1), columns(h1)
    alpha, rest = solve(g1_cols, [own_gram, h1])
    alpha_t, rest_t = columns_t(alpha), columns_t(rest)
    beta = own_gram - times(g1_cols, alpha)
    beta = beta + times(alpha_t, times(columns(g2), alpha) - g1)
    own_cols = columns(own_gram)
    (beta,) = solve(own_cols, [beta])
    mix = rest + beta
    mix_t = columns_t(mix)
    g1_mix = times(g1_cols, mix)
    early = times(own_cols, rest) - times(h1_cols, alpha)
    early = times(rest_t, early) - times(alpha_t, times(h1_cols, rest))

    def put_table(dst, base, m):
        for i in range(N):
            line = splat_row(m, i)
            for j in range(N):
                dst[base + N * j + i] = splat_col(line, j)

    put_table(TA, 0, alpha)
    put_table(TA, 64, unit + beta)

    def second_body(j, carry):
        a = [TA[N * j + i] for i in range(N)]
        b = [TA[64 + N * j + i] for i in range(N)]

        def body(x, carry):
            for t in range(4):
                at = pl.ds(8 * t, 8)
                r = [row(V, f, x, t) for f in range(N)]
                q = [row(Q, f, x, t) for f in range(N)]
                s = [S[f, x, at] for f in range(N)]

                def comb(c, v):
                    total = c[0] * v[0]
                    for i in range(1, N):
                        total = total + c[i] * v[i]
                    return total

                aq = comb(a, q)
                X1[j, x, at] = comb(a, r)
                R1[j, x, at] = row(V, j, x, t) - aq
                D2[j, x, at] = comb(b, r) - aq
                A2[j, x, at] = comb(b, q) - comb(a, s)
            return carry

        lax.fori_loop(0, 16, body, 0)
        return carry

    lax.fori_loop(0, 2, second_body, 0)
    reduce_start(1, 1, reduce_finish(1, 0))
    lax.fori_loop(2, N, second_body, 0)
    sum2 = reduce_finish(1, 1)

    h2_cols, zs_cols = columns(sum2), columns(sum2, 8)
    norm_next = early + times(alpha_t, times(h2_cols, alpha))
    cross = [h + theta * g for h, g in zip(h2_cols, h1_cols)]
    h3_cols = [z - theta * c for z, c in zip(zs_cols, cross)]
    curve = times(mix_t, g1_mix - times(cross, alpha)) + times(
        alpha_t, times(h3_cols, alpha) - times(cross, mix)
    )
    (alpha2,) = solve(columns(curve), [norm_next])
    put_table(T, 0, alpha2)

    for d in flat:
        sent_if(d, field_part(d, V, send1, recv1))
        sent_if(d, field_part(d, Q, send2, recv2))
    for d in flat_w:
        sent_if(d, weight_part(d))
    for d in cols:
        sent_if(d, column_part(d, True))
        sent_if(d, column_part(d, False))
    for which in range(2):
        for step in range(2):
            for copy in reduce_copies(which, step):
                copy.wait_send()


def finish_kernel(X1, R1, D2, A2, T, x_out, r_out, X, Y, sems):
    def store(j):
        return [
            pltpu.make_async_copy(buf.at[j], out.at[j], sems.at[k, j])
            for k, (buf, out) in enumerate(((X, x_out), (Y, r_out)))
        ]

    for pair in range(0, N, 2):
        js = (pair, pair + 1)
        a = {j: [T[N * j + i] for i in range(N)] for j in js}

        def body(p, carry):
            for t in range(4):
                at = pl.ds(8 * t, 8)
                d = [D2[i, p, at] for i in range(N)]
                e = [A2[i, p, at] for i in range(N)]
                for j in js:
                    x = X1[j, p, at]
                    res = R1[j, p, at]
                    for i in range(0, N, 2):
                        x = x + (a[j][i] * d[i] + a[j][i + 1] * d[i + 1])
                        res = res - (a[j][i] * e[i] + a[j][i + 1] * e[i + 1])
                    X[j, p, at] = x
                    Y[j, p, at] = res
            return carry

        lax.fori_loop(0, 16, body, 0)
        for j in js:
            for copy in store(j):
                copy.start()
    for j in range(N):
        for copy in store(j):
            copy.wait()


def shards(sizes, rhs, stencil):
    nx, ny, nz = sizes
    block = rhs.shape
    anyspace = pl.BlockSpec(memory_space=pl.ANY)
    local = pl.BlockSpec(memory_space=pltpu.VMEM)
    hbm = pl.BlockSpec(memory_space=pltpu.HBM)
    field = jax.ShapeDtypeStruct(block, F32)
    kept = pl.pallas_call(
        functools.partial(kernel, sizes),
        out_shape=(field,) * 4 + (jax.ShapeDtypeStruct((64, 8, 128), F32),),
        in_specs=[hbm, hbm],
        out_specs=(local,) * 5,
        scratch_shapes=[
            pltpu.VMEM((8, 18, 48, 128), F32),
            pltpu.VMEM((8, 18, 48, 128), F32),
            pltpu.VMEM(block, F32),
            pltpu.VMEM((128, 8, 128), F32),
            pltpu.VMEM((14, 17, 48, 128), F32),
            pltpu.VMEM((16, 32, 128), F32),
            pltpu.VMEM((10, 16, 32, 128), F32),
            pltpu.VMEM((9, 16, 32, 128), F32),
            pltpu.VMEM((16, 32, 128), F32),
            pltpu.VMEM((2, 2, 32, 128), F32),
            pltpu.VMEM((2, 2, 4, 48, 128), F32),
            pltpu.VMEM((2, 32, 128), F32),
            pltpu.VMEM((2, 4, 48, 128), F32),
            pltpu.VMEM((18, 48, 128), F32),
            pltpu.VMEM((17, 48, 128), F32),
            pltpu.VMEM((2, 2, 8, 128), F32),
            pltpu.VMEM((2, ny + nx * nz, 8, 128), F32),
            pltpu.SemaphoreType.DMA((2,)),
            pltpu.SemaphoreType.DMA((31,)),
            pltpu.SemaphoreType.DMA((31,)),
            pltpu.SemaphoreType.DMA((26,)),
            pltpu.SemaphoreType.DMA((26,)),
            pltpu.SemaphoreType.DMA((2, ny + nx * nz)),
            pltpu.SemaphoreType.DMA((2, ny + nx * nz)),
        ],
        compiler_params=pltpu.CompilerParams(
            collective_id=0, has_side_effects=True, vmem_limit_bytes=44 * 2**20
        ),
        name="operator",
    )(rhs, stencil)
    return pl.pallas_call(
        finish_kernel,
        out_shape=(jax.ShapeDtypeStruct(block, F32), jax.ShapeDtypeStruct(block, F32)),
        in_specs=[local] * 5,
        out_specs=(anyspace, anyspace),
        scratch_shapes=[
            pltpu.VMEM(block, F32),
            pltpu.VMEM(block, F32),
            pltpu.SemaphoreType.DMA((2, N)),
        ],
        compiler_params=pltpu.CompilerParams(vmem_limit_bytes=24 * 2**20),
        name="finish",
    )(*kept)


def solution(mesh):
    sizes = tuple(mesh.shape[n] for n in ("gx", "gy", "gz"))
    placed = P(None, "gx", "gy", "gz")
    return jax.shard_map(
        functools.partial(shards, sizes),
        mesh=mesh,
        in_specs=(placed, placed),
        out_specs=(placed, placed),
        check_vma=False,
    )
```

```python
import functools

import jax
import jax.numpy as jnp
from jax import lax
from jax.experimental import pallas as pl
from jax.experimental.pallas import tpu as pltpu
from jax.sharding import PartitionSpec as P

F32 = jnp.float32
N = 8
FORWARD = [
    (a, b, c) for a in (-1, 0, 1) for b in (-1, 0, 1) for c in (-1, 0, 1) if (a, b, c) > (0, 0, 0)
]
INDEX = {o: k + 1 for k, o in enumerate(FORWARD)}
PLANE = [(a, b) for a in (-1, 0, 1) for b in (-1, 0, 1)]
SLOTS = [(0, 0), (0, 1), (1, -1), (1, 0), (1, 1)]
LOW = [INDEX[(a, b, 1)] for a, b in SLOTS]
UP = [INDEX[(a, b, -1)] if (a, b) != (0, 0) else INDEX[(0, 0, 1)] for a, b in SLOTS]
DIRS = [
    (a, b, c) for a in (-1, 0, 1) for b in (-1, 0, 1) for c in (-1, 0, 1) if (a, b, c) != (0, 0, 0)
]
WRANGE = {(1, 0): (5, 9), (1, 1): (11, 3), (1, -1): (5, 3), (0, 1): (2, 12), (0, -1): (5, 3)}
WDIRS = list(WRANGE)
PAIRS = [(i, j) for i in range(N) for j in range(i, N)]
TOP = 8


def lanes():
    return lax.broadcasted_iota(jnp.int32, (8, 128), 1)


def rows():
    return lax.broadcasted_iota(jnp.int32, (8, 128), 0)


def splat_row(m, k):
    return jnp.broadcast_to(m[k : k + 1, :], (8, 128))


def splat_col(m, k):
    return jnp.broadcast_to(m[:, k : k + 1], (8, 128))


def row_sum(m):
    return jnp.broadcast_to(jnp.sum(m, axis=1, keepdims=True), (8, 128))


def shift(m, amount):
    amount = amount % 128
    return pltpu.roll(m, amount, 1) if amount else m


def columns(m, base=0):
    return [splat_col(m, base + k) for k in range(N)]


def columns_t(m):
    same = lanes() == rows()
    return [row_sum(jnp.where(same, splat_row(m, k), 0.0)) for k in range(N)]


def times(cols, m):
    terms = [cols[k] * splat_row(m, k) for k in range(N)]
    while len(terms) > 1:
        terms = [a + b for a, b in zip(terms[::2], terms[1::2])]
    return terms[0]


def solve(cols, rights):
    cols = list(cols)
    row_id = rows()
    for k in range(N):
        here = row_id == k
        inverse = 1.0 / splat_row(cols[k], k)
        factor = cols[k] * inverse

        def step(m):
            line = splat_row(m, k)
            return jnp.where(here, line * inverse, m - factor * line)

        cols = cols[: k + 1] + [step(c) for c in cols[k + 1 :]]
        rights = [step(r) for r in rights]
    return rights


def kernel(
    sizes,
    x_ref,
    w_ref,
    X1,
    R1,
    D2,
    A2,
    T,
    V,
    Q,
    S,
    TA,
    W,
    PX,
    WW,
    WE,
    R,
    PP,
    LPP,
    PQ,
    LPQ,
    G,
    GW,
    ARS,
    ARL,
    load_sem,
    send1,
    recv1,
    send2,
    recv2,
    ar_send,
    ar_recv,
):
    names = ("gx", "gy", "gz")
    nx, ny, nz = sizes
    me = tuple(lax.axis_index(n) for n in names)

    def exists(d):
        cond = None
        for pos, step, count in zip(me, d, sizes):
            term = None
            if step > 0:
                term = pos < count - 1
            elif step < 0:
                term = pos > 0
            if term is not None:
                cond = term if cond is None else cond & term
        return cond

    def opposite(d):
        return tuple(-t for t in d)

    def target(d):
        return tuple(pos + step for pos, step in zip(me, d))

    groups = ((1,), (0, 2))
    offsets = (
        [(0, p, 0) for p in range(1, ny)],
        [(p, 0, r) for p in range(nx) for r in range(nz) if p or r],
    )
    own_slot = (me[1], ny + me[0] * nz + me[2])
    slots = ((0, ny), (ny, nx * nz))

    def peer(d):
        return tuple(lax.rem(pos + p, n) if p else pos for pos, p, n in zip(me, d, sizes))

    load_x = pltpu.make_async_copy(x_ref, V.at[:, pl.ds(1, 16), pl.ds(TOP, 32)], load_sem.at[0])
    load_w = pltpu.make_async_copy(w_ref, W.at[:, pl.ds(1, 16), pl.ds(TOP, 32)], load_sem.at[1])
    load_x.start()
    load_w.start()

    zero = jnp.zeros((8, 128), F32)

    def clear_padded(buf, first, last):
        for field in range(buf.shape[0]):
            for plane in (first, last):
                if plane is not None:
                    for t in range(6):
                        buf[field, plane, pl.ds(8 * t, 8)] = zero

        def body(p, carry):
            for field in range(buf.shape[0]):
                buf[field, p, pl.ds(0, 8)] = zero
                buf[field, p, pl.ds(40, 8)] = zero
            return carry

        lax.fori_loop(1, 17, body, 0)

    clear_padded(V, 0, 17)
    clear_padded(Q, 0, 17)
    clear_padded(W, 0, None)

    def clear_landing(i, carry):
        for t in range(6):
            for s in range(2):
                for k in range(2):
                    LPP[s, k, i, pl.ds(8 * t, 8)] = zero
                LPQ[s, i, pl.ds(8 * t, 8)] = zero
        return carry

    lax.fori_loop(0, 4, clear_landing, 0)

    barrier = pltpu.get_barrier_semaphore()
    for d in DIRS:

        @pl.when(exists(d))
        def _():
            pl.semaphore_signal(
                barrier, inc=1, device_id=target(d), device_id_type=pl.DeviceIdType.MESH
            )

    for step in range(2):
        for d in offsets[step]:
            pl.semaphore_signal(
                barrier, inc=1, device_id=peer(d), device_id_type=pl.DeviceIdType.MESH
            )
    span = []
    for pos, count in zip(me, sizes):
        span.append(1 + (pos > 0).astype(jnp.int32) + (pos < count - 1).astype(jnp.int32))
    def along(step, whole, plus, minus):
        if step == 0:
            return (pl.ds(*whole), pl.ds(*whole))
        src, dst = plus if step > 0 else minus
        return (pl.ds(src, 1), pl.ds(dst, 1))

    def field_part(d, buf, sends, recvs):
        i = DIRS.index(d)
        xs, xd = along(d[0], (1, 16), (16, 0), (1, 17))
        ys, yd = along(d[1], (TOP, 32), (TOP + 31, TOP - 1), (TOP, TOP + 32))
        return pltpu.make_async_remote_copy(
            src_ref=buf.at[:, xs, ys],
            dst_ref=buf.at[:, xd, yd],
            send_sem=sends.at[i],
            recv_sem=recvs.at[i],
            device_id=target(d),
            device_id_type=pl.DeviceIdType.MESH,
        )

    def weight_part(d):
        i = 26 + WDIRS.index((d[0], d[1]))
        k0, kn = WRANGE[(d[0], d[1])]
        xs, xd = along(d[0], (1, 16), (16, 0), (1, 17))
        ys, yd = along(d[1], (TOP, 32), (TOP + 31, TOP - 1), (TOP, TOP + 32))
        return pltpu.make_async_remote_copy(
            src_ref=W.at[pl.ds(k0, kn), xs, ys],
            dst_ref=W.at[pl.ds(k0, kn), xd, yd],
            send_sem=send1.at[i],
            recv_sem=recv1.at[i],
            device_id=target(d),
            device_id_type=pl.DeviceIdType.MESH,
        )

    def column_part(d, both):
        i = DIRS.index(d)
        side = 0 if d[2] > 0 else 1
        if d[0] == 0:
            gs, gd = pl.ds(0, 2), pl.ds(1, 2)
        elif d[0] > 0:
            gs, gd = pl.ds(1, 1), pl.ds(0, 1)
        else:
            gs, gd = pl.ds(0, 1), pl.ds(3, 1)
        if d[1] == 0:
            ys, yd = pl.ds(0, 32), pl.ds(TOP, 32)
        elif d[1] > 0:
            ys, yd = pl.ds(31, 1), pl.ds(TOP - 1, 1)
        else:
            ys, yd = pl.ds(0, 1), pl.ds(TOP + 32, 1)
        src = PP.at[:, gs, ys] if both else PQ.at[gs, ys]
        dst = LPP.at[side, :, gd, yd] if both else LPQ.at[side, gd, yd]
        return pltpu.make_async_remote_copy(
            src_ref=src,
            dst_ref=dst,
            send_sem=(send1 if both else send2).at[i],
            recv_sem=(recv1 if both else recv2).at[i],
            device_id=target(d),
            device_id_type=pl.DeviceIdType.MESH,
        )

    def start_if(d, copy):
        @pl.when(exists(d))
        def _():
            copy.start()

    def recv_if(d, copy):
        @pl.when(exists(opposite(d)))
        def _():
            copy.wait_recv()

    def sent_if(d, copy):
        @pl.when(exists(d))
        def _():
            copy.wait_send()

    flat = sorted((d for d in DIRS if d[2] == 0), key=lambda d: abs(d[1]))
    flat_w = [(a, b, 0) for a, b in WDIRS]
    cols = [d for d in DIRS if d[2] != 0]

    lane = lanes()
    odd = lax.rem(lane, 2) == 1
    first = lane == 0
    last = lane == 127
    half = lane // 2

    def gather_columns(fields):
        total = zero
        for slot, v in enumerate(fields):
            total = jnp.where(half == slot, shift(v, 2 * slot + 1), total)
        return total

    def merge_columns(dst):
        for xg in range(2):
            for t in range(4):
                at = pl.ds(8 * t, 8)
                parts = [
                    jnp.where(lane // 16 == xm, shift(PX[xg * 8 + xm, at], 16 * xm), 0.0)
                    for xm in range(8)
                ]
                while len(parts) > 1:
                    parts = [a + b for a, b in zip(parts[::2], parts[1::2])]
                dst(xg, at, parts[0])

    def pack(dst, group):
        def body(i, carry):
            for k in range(4):
                x = 4 * i + k
                for t in range(4):
                    PX[x, pl.ds(8 * t, 8)] = gather_columns(
                        group(x + 1, pl.ds(TOP + 8 * t, 8))
                    )
            return carry

        lax.fori_loop(0, 4, body, 0)
        merge_columns(dst)

    def put_weights(xg, at, total):
        PP[1, xg, at] = total

    def weight_group(p, at):
        return [jnp.where(first, W[UP[j], p, at], W[LOW[j], p, at]) for j in range(5)]

    def unpack(get, dst, planes):
        for t in range(6):
            r0 = 8 * t
            merged = {}
            for xi in planes:
                if xi == 0:
                    g, off = 0, 112
                elif xi == 17:
                    g, off = 3, 0
                else:
                    g, off = 1 + (xi - 1) // 8, 16 * ((xi - 1) % 8)
                if g not in merged:
                    merged[g] = jnp.where(odd, get(1, g, r0), get(0, g, r0))
                dst[xi, pl.ds(r0, 8)] = shift(merged[g], -off)

    def blocks(body, first_x, count, width):
        def several(i, carry):
            for k in range(width):
                body(first_x + width * i + k, carry)
            return carry

        lax.fori_loop(0, count, several, 0)

    flat_y = [d for d in flat if d[0] == 0]
    flat_x = [d for d in flat if d[0] != 0]
    flat_wy = [d for d in flat_w if d[0] == 0]
    flat_wx = [d for d in flat_w if d[0] != 0]
    cols_y = [d for d in cols if d[0] == 0]
    cols_x = [d for d in cols if d[0] != 0]

    def put_pp(xg, at, total):
        PP[0, xg, at] = total

    load_x.wait()
    pack(put_pp, lambda p, at: [V[f, p, at] for f in range(N)])
    load_w.wait()
    pack(put_weights, weight_group)

    pl.semaphore_wait(
        barrier, span[0] * span[1] * span[2] - 1 + (ny - 1) + (nx * nz - 1)
    )

    for d in flat_y:
        start_if(d, field_part(d, V, send1, recv1))
    for d in flat_wy:
        start_if(d, weight_part(d))
    for d in cols_y:
        start_if(d, column_part(d, True))
    for d in flat_x:
        start_if(d, field_part(d, V, send1, recv1))
    for d in cols_x:
        start_if(d, column_part(d, True))
    for d in flat_wx:
        start_if(d, weight_part(d))

    def m_of(a, b):
        return 3 * (a + 1) + (b + 1)

    def spread_columns(v, even_from, odd_from):
        return jnp.take_along_axis(v, jnp.where(odd, odd_from, even_from), axis=1)

    def prepare_own(x, carry):
        for t in range(4):
            out = pl.ds(8 * t, 8)
            own = [W[k, x + 1, pl.ds(TOP + 8 * t, 8)] for k in range(14)]
            diag = (own[0] + own[1]) + (own[2] + own[3])
            for k in range(4, 14, 2):
                diag = diag + (own[k] + own[k + 1])
            WW[0, x, out] = diag
            for j, (a, b) in enumerate(SLOTS):
                WW[1 + j, x, out] = shift(own[LOW[j]], 1)
                if j:
                    WW[5 + j, x, out] = shift(own[UP[j]], 127)
                    WE[m_of(a, b), x, out] = spread_columns(
                        jnp.where(first, own[UP[j]], own[LOW[j]]), 0, 127
                    )
        return carry

    def prepare(x, carry):
        for t in range(4):
            r0 = TOP + 8 * t

            def w_at(k, a=0, b=0):
                return W[k, x + 1 + a, pl.ds(r0 + b, 8)]

            out = pl.ds(8 * t, 8)
            diag = WW[0, x, out]
            ahead = zero
            behind = w_at(LOW[0])
            own = spread_columns(
                jnp.where(last, behind, GW[x + 1, pl.ds(r0, 8)]), 0, 127
            )
            WE[m_of(0, 0), x, out] = own
            edge = jnp.where(odd, 0.0, own)
            for j, (a, b) in enumerate(SLOTS):
                if j == 0:
                    continue
                back = spread_columns(GW[x + 1 - a, pl.ds(r0 - b, 8)], 2 * j, 2 * j + 1)
                WE[m_of(-a, -b), x, out] = back
                edge = edge + back
                diag = diag + w_at(INDEX[(a, b, 0)], -a, -b)
                ahead = ahead + w_at(UP[j], -a, -b)
                behind = behind + w_at(LOW[j], -a, -b)
            diag = diag + jnp.where(last, edge, shift(ahead, 127))
            diag = diag + jnp.where(first, edge, shift(behind, 1))
            WW[0, x, out] = diag
        return carry

    blocks(prepare_own, 0, 8, 2)

    def gram_loop(get):
        sums = []
        for lo, hi in ((0, 3), (3, N)):
            pairs = [(i, j) for i, j in PAIRS if lo <= i < hi]

            def body(planes, acc):
                acc = list(acc)
                for k in range(8):
                    x, t = 2 * planes + k // 4, k % 4
                    left, right = get(x, t, range(lo, hi), range(lo, N))
                    for n, (i, j) in enumerate(pairs):
                        acc[n] = acc[n] + left[i] * right[j]
                return tuple(acc)

            sums += list(lax.fori_loop(0, 8, body, tuple(zero for _ in pairs)))
        return sums

    def spread(parts, acc, offset):
        for n, (i, j) in enumerate(PAIRS):
            total = row_sum(acc[n])
            parts[i] = jnp.where(lane == offset + j, total, parts[i])
            if i != j:
                parts[j] = jnp.where(lane == offset + i, total, parts[j])
        return parts

    def fold(parts):
        result = zero
        for i in range(N):
            total = jnp.broadcast_to(jnp.sum(parts[i], axis=0, keepdims=True), (8, 128))
            result = jnp.where(rows() == i, total, result)
        return result

    def row(buf, f, x, t):
        return buf[f, x + 1, pl.ds(TOP + 8 * t, 8)]

    def get_rr(x, t, left, right):
        v = {f: row(V, f, x, t) for f in right}
        return v, v

    parts1 = spread([zero] * N, gram_loop(get_rr), 0)

    for d in flat_y:
        recv_if(d, field_part(d, V, send1, recv1))
    for d in flat_wy:
        recv_if(d, weight_part(d))
    for d in cols_y:
        recv_if(d, column_part(d, True))

    def get_lpp(k):
        return lambda s, g, r0: LPP[s, k, g, pl.ds(r0, 8)]

    def get_lpq(s, g, r0):
        return LPQ[s, g, pl.ds(r0, 8)]

    unpack(get_lpp(0), G, range(1, 17))
    unpack(get_lpp(1), GW, range(1, 17))

    def edges(x, carry):
        for t in range(4):
            total = zero
            for a, b in PLANE:
                total = total + WE[m_of(a, b), x, pl.ds(8 * t, 8)] * G[
                    x + 1 + a, pl.ds(TOP + 8 * t + b, 8)
                ]
            R[x, pl.ds(8 * t, 8)] = total
        return carry

    def coupling(x, t, a, b, c):
        j = SLOTS.index((a, b)) if (a, b) in SLOTS else SLOTS.index((-a, -b))
        here = pl.ds(8 * t, 8)
        away = W.at[:, x + 1 + a, pl.ds(TOP + 8 * t + b, 8)]
        ahead = (a, b) in SLOTS
        if c == 0:
            if (a, b) == (0, 0):
                return WW[0, x, here]
            if ahead:
                return W[INDEX[(a, b, 0)], x + 1, pl.ds(TOP + 8 * t, 8)]
            return away[INDEX[(-a, -b, 0)]]
        if c == 1:
            return WW[1 + j, x, here] if ahead else away[UP[j]]
        if ahead and j:
            return WW[5 + j, x, here]
        return away[LOW[j]]

    def operate(src, put):
        def body(x, carry):
            for t in range(4):
                halo = R[x, pl.ds(8 * t, 8)]
                for group in (range(0, 4), range(4, N)):
                    centre = {}
                    sums = {f: [None, None, None] for f in group}
                    for a, b in PLANE:
                        weights = [coupling(x, t, a, b, c) for c in (0, 1, -1)]
                        for f in group:
                            v = src[f, x + 1 + a, pl.ds(TOP + 8 * t + b, 8)]
                            for c in range(3):
                                term = weights[c] * v
                                if c == 0 and (a, b) == (0, 0):
                                    centre[f] = term
                                elif sums[f][c] is None:
                                    sums[f][c] = term
                                else:
                                    sums[f][c] = sums[f][c] + term
                    for f in group:
                        side = shift(halo, -(2 * f + 1))
                        total = centre[f] - sums[f][0]
                        total = total - shift(jnp.where(first, side, sums[f][1]), 127)
                        total = total - shift(jnp.where(last, side, sums[f][2]), 1)
                        put(f, x, t, total)
            return carry

        return body

    def ends(body):
        lax.fori_loop(0, 2, lambda i, carry: body(15 * i, carry), 0)

    def put_q(f, x, t, value):
        Q[f, x + 1, pl.ds(TOP + 8 * t, 8)] = value

    def put_s(f, x, t, value):
        S[f, x, pl.ds(8 * t, 8)] = value

    blocks(prepare, 1, 5, 3)
    blocks(edges, 1, 7, 2)
    blocks(operate(V, put_q), 1, 14, 1)
    for d in flat_x:
        recv_if(d, field_part(d, V, send1, recv1))
    for d in flat_wx:
        recv_if(d, weight_part(d))
    for d in cols_x:
        recv_if(d, column_part(d, True))
    unpack(get_lpp(0), G, (0, 17))
    unpack(get_lpp(1), GW, (0,))
    prepare(0, 0)
    ends(edges)
    ends(operate(V, put_q))

    for d in flat_y + flat_x:
        start_if(d, field_part(d, Q, send2, recv2))

    def put_pq(xg, at, total):
        PQ[xg, at] = total

    pack(put_pq, lambda p, at: [Q[f, p, at] for f in range(N)])
    for d in cols_y + cols_x:
        start_if(d, column_part(d, False))

    def reduce_copies(which, step):
        copies = []
        for i, d in enumerate(offsets[step]):
            i = slots[step][0] + i
            copies.append(
                pltpu.make_async_remote_copy(
                    src_ref=ARS.at[which, step],
                    dst_ref=ARL.at[which, own_slot[step]],
                    send_sem=ar_send.at[which, i],
                    recv_sem=ar_recv.at[which, i],
                    device_id=peer(d),
                    device_id_type=pl.DeviceIdType.MESH,
                )
            )
        return copies

    def reduce_start(which, step, value):
        ARS[which, step] = value
        ARL[which, own_slot[step]] = value
        for copy in reduce_copies(which, step):
            copy.start()

    def reduce_finish(which, step):
        for copy in reduce_copies(which, step):
            copy.wait_recv()
        lo, count = slots[step]
        parts = [ARL[which, lo + i] for i in range(count)]
        while len(parts) > 1:
            parts = [a + b for a, b in zip(parts[::2], parts[1::2])]
        return parts[0]

    def get_rq(x, t, left, right):
        return (
            {f: row(V, f, x, t) for f in left},
            {f: row(Q, f, x, t) for f in right},
        )

    def get_qq(x, t, left, right):
        q = {f: row(Q, f, x, t) for f in right}
        return q, q

    parts1 = spread(parts1, gram_loop(get_rq), 8)
    parts1 = spread(parts1, gram_loop(get_qq), 16)
    reduce_start(0, 0, fold(parts1))

    for d in flat_y:
        recv_if(d, field_part(d, Q, send2, recv2))
    for d in cols_y:
        recv_if(d, column_part(d, False))
    unpack(get_lpq, G, range(1, 17))
    blocks(edges, 1, 7, 2)
    blocks(operate(Q, put_s), 1, 4, 1)
    reduce_start(0, 1, reduce_finish(0, 0))
    blocks(operate(Q, put_s), 5, 10, 1)
    for d in flat_x:
        recv_if(d, field_part(d, Q, send2, recv2))
    for d in cols_x:
        recv_if(d, column_part(d, False))
    unpack(get_lpq, G, (0, 17))
    ends(edges)
    ends(operate(Q, put_s))
    sum1 = reduce_finish(0, 1)

    def trace(m):
        total = row_sum(jnp.where(lane == rows(), m, 0.0))
        return jnp.broadcast_to(jnp.sum(total, axis=0, keepdims=True), (8, 128))

    small = lane < 8
    own_gram = jnp.where(small, sum1, 0.0)
    g1 = jnp.where(small, shift(sum1, -8), 0.0)
    g2 = shift(sum1, -16)
    theta = trace(g1) / trace(own_gram)
    h1 = g1 - theta * own_gram

    def moved(f, x, t):
        return row(Q, f, x, t) - theta * row(V, f, x, t)

    def get_h2(x, t, left, right):
        z = {f: moved(f, x, t) for f in right}
        return z, z

    def get_zs(x, t, left, right):
        return (
            {f: moved(f, x, t) for f in left},
            {f: S[f, x, pl.ds(8 * t, 8)] for f in right},
        )

    parts2 = [zero] * N
    parts2 = spread(parts2, gram_loop(get_h2), 0)
    parts2 = spread(parts2, gram_loop(get_zs), 8)
    reduce_start(1, 0, fold(parts2))

    unit = jnp.where(lane == rows(), 1.0, 0.0)
    g1_cols, h1_cols = columns(g1), columns(h1)
    alpha, rest = solve(g1_cols, [own_gram, h1])
    alpha_t, rest_t = columns_t(alpha), columns_t(rest)
    beta = own_gram - times(g1_cols, alpha)
    beta = beta + times(alpha_t, times(columns(g2), alpha) - g1)
    own_cols = columns(own_gram)
    (beta,) = solve(own_cols, [beta])
    mix = rest + beta
    mix_t = columns_t(mix)
    g1_mix = times(g1_cols, mix)
    early = times(own_cols, rest) - times(h1_cols, alpha)
    early = times(rest_t, early) - times(alpha_t, times(h1_cols, rest))

    def put_table(dst, base, m):
        for i in range(N):
            line = splat_row(m, i)
            for j in range(N):
                dst[base + N * j + i] = splat_col(line, j)

    put_table(TA, 0, alpha)
    put_table(TA, 64, unit + beta)

    def second_body(j, carry):
        a = [TA[N * j + i] for i in range(N)]
        b = [TA[64 + N * j + i] for i in range(N)]

        def body(x, carry):
            for t in range(4):
                at = pl.ds(8 * t, 8)
                r = [row(V, f, x, t) for f in range(N)]
                q = [row(Q, f, x, t) for f in range(N)]
                s = [S[f, x, at] for f in range(N)]

                def comb(c, v):
                    total = c[0] * v[0]
                    for i in range(1, N):
                        total = total + c[i] * v[i]
                    return total

                aq = comb(a, q)
                X1[j, x, at] = comb(a, r)
                R1[j, x, at] = row(V, j, x, t) - aq
                D2[j, x, at] = comb(b, r) - aq
                A2[j, x, at] = comb(b, q) - comb(a, s)
            return carry

        lax.fori_loop(0, 16, body, 0)
        return carry

    lax.fori_loop(0, 2, second_body, 0)
    reduce_start(1, 1, reduce_finish(1, 0))
    lax.fori_loop(2, N, second_body, 0)
    for d in flat:
        sent_if(d, field_part(d, V, send1, recv1))
        sent_if(d, field_part(d, Q, send2, recv2))
    for d in flat_w:
        sent_if(d, weight_part(d))
    for d in cols:
        sent_if(d, column_part(d, True))
        sent_if(d, column_part(d, False))
    for copy in reduce_copies(0, 0) + reduce_copies(0, 1):
        copy.wait_send()
    sum2 = reduce_finish(1, 1)

    h2_cols, zs_cols = columns(sum2), columns(sum2, 8)
    norm_next = early + times(alpha_t, times(h2_cols, alpha))
    cross = [h + theta * g for h, g in zip(h2_cols, h1_cols)]
    h3_cols = [z - theta * c for z, c in zip(zs_cols, cross)]
    curve = times(mix_t, g1_mix - times(cross, alpha)) + times(
        alpha_t, times(h3_cols, alpha) - times(cross, mix)
    )
    (alpha2,) = solve(columns(curve), [norm_next])
    put_table(T, 0, alpha2)

    for copy in reduce_copies(1, 0) + reduce_copies(1, 1):
        copy.wait_send()


def finish_kernel(X1, R1, D2, A2, T, x_out, r_out, X, Y, sems):
    def store(j, lo, count):
        at = pl.ds(lo, count)
        return [
            pltpu.make_async_copy(
                buf.at[j, at], out.at[j, at], sems.at[k, j + lo // 4]
            )
            for k, (buf, out) in enumerate(((X, x_out), (Y, r_out)))
        ]

    started = []
    for pair in range(0, N, 2):
        js = (pair, pair + 1)
        a = {j: [T[N * j + i] for i in range(N)] for j in js}

        def body(planes, carry):
            for k in range(8):
                p = 2 * planes + k // 4
                at = pl.ds(8 * (k % 4), 8)
                d = [D2[i, p, at] for i in range(N)]
                e = [A2[i, p, at] for i in range(N)]
                for j in js:
                    x = X1[j, p, at]
                    res = R1[j, p, at]
                    for i in range(0, N, 2):
                        x = x + (a[j][i] * d[i] + a[j][i + 1] * d[i + 1])
                        res = res - (a[j][i] * e[i] + a[j][i + 1] * e[i + 1])
                    X[j, p, at] = x
                    Y[j, p, at] = res
            return carry

        for lo, count in ((0, 16),) if pair < 6 else ((0, 8), (8, 8)):
            lax.fori_loop(lo // 2, (lo + count) // 2, body, 0)
            for j in js:
                for copy in store(j, lo, count):
                    copy.start()
                    started.append(copy)
    for copy in started:
        copy.wait()


def shards(sizes, rhs, stencil):
    nx, ny, nz = sizes
    block = rhs.shape
    anyspace = pl.BlockSpec(memory_space=pl.ANY)
    local = pl.BlockSpec(memory_space=pltpu.VMEM)
    hbm = pl.BlockSpec(memory_space=pltpu.HBM)
    field = jax.ShapeDtypeStruct(block, F32)
    kept = pl.pallas_call(
        functools.partial(kernel, sizes),
        out_shape=(field,) * 4 + (jax.ShapeDtypeStruct((64, 8, 128), F32),),
        in_specs=[hbm, hbm],
        out_specs=(local,) * 5,
        scratch_shapes=[
            pltpu.VMEM((8, 18, 48, 128), F32),
            pltpu.VMEM((8, 18, 48, 128), F32),
            pltpu.VMEM(block, F32),
            pltpu.VMEM((128, 8, 128), F32),
            pltpu.VMEM((14, 17, 48, 128), F32),
            pltpu.VMEM((16, 32, 128), F32),
            pltpu.VMEM((10, 16, 32, 128), F32),
            pltpu.VMEM((9, 16, 32, 128), F32),
            pltpu.VMEM((16, 32, 128), F32),
            pltpu.VMEM((2, 2, 32, 128), F32),
            pltpu.VMEM((2, 2, 4, 48, 128), F32),
            pltpu.VMEM((2, 32, 128), F32),
            pltpu.VMEM((2, 4, 48, 128), F32),
            pltpu.VMEM((18, 48, 128), F32),
            pltpu.VMEM((17, 48, 128), F32),
            pltpu.VMEM((2, 2, 8, 128), F32),
            pltpu.VMEM((2, ny + nx * nz, 8, 128), F32),
            pltpu.SemaphoreType.DMA((2,)),
            pltpu.SemaphoreType.DMA((31,)),
            pltpu.SemaphoreType.DMA((31,)),
            pltpu.SemaphoreType.DMA((26,)),
            pltpu.SemaphoreType.DMA((26,)),
            pltpu.SemaphoreType.DMA((2, ny + nx * nz)),
            pltpu.SemaphoreType.DMA((2, ny + nx * nz)),
        ],
        compiler_params=pltpu.CompilerParams(
            collective_id=0, has_side_effects=True, vmem_limit_bytes=44 * 2**20
        ),
        name="operator",
    )(rhs, stencil)
    return pl.pallas_call(
        finish_kernel,
        out_shape=(jax.ShapeDtypeStruct(block, F32), jax.ShapeDtypeStruct(block, F32)),
        in_specs=[local] * 5,
        out_specs=(anyspace, anyspace),
        scratch_shapes=[
            pltpu.VMEM(block, F32),
            pltpu.VMEM(block, F32),
            pltpu.SemaphoreType.DMA((2, N + 2)),
        ],
        compiler_params=pltpu.CompilerParams(vmem_limit_bytes=24 * 2**20),
        name="finish",
    )(*kept)


def solution(mesh):
    sizes = tuple(mesh.shape[n] for n in ("gx", "gy", "gz"))
    placed = P(None, "gx", "gy", "gz")
    return jax.shard_map(
        functools.partial(shards, sizes),
        mesh=mesh,
        in_specs=(placed, placed),
        out_specs=(placed, placed),
        check_vma=False,
    )
```

```python
import functools

import jax
import jax.numpy as jnp
from jax import lax
from jax.experimental import pallas as pl
from jax.experimental.pallas import tpu as pltpu
from jax.sharding import PartitionSpec as P

F32 = jnp.float32
N = 8
FORWARD = [
    (a, b, c) for a in (-1, 0, 1) for b in (-1, 0, 1) for c in (-1, 0, 1) if (a, b, c) > (0, 0, 0)
]
INDEX = {o: k + 1 for k, o in enumerate(FORWARD)}
PLANE = [(a, b) for a in (-1, 0, 1) for b in (-1, 0, 1)]
SLOTS = [(0, 0), (0, 1), (1, -1), (1, 0), (1, 1)]
LOW = [INDEX[(a, b, 1)] for a, b in SLOTS]
UP = [INDEX[(a, b, -1)] if (a, b) != (0, 0) else INDEX[(0, 0, 1)] for a, b in SLOTS]
DIRS = [
    (a, b, c) for a in (-1, 0, 1) for b in (-1, 0, 1) for c in (-1, 0, 1) if (a, b, c) != (0, 0, 0)
]
WRANGE = {(1, 0): (5, 9), (1, 1): (11, 3), (1, -1): (5, 3), (0, 1): (2, 12), (0, -1): (5, 3)}
WDIRS = list(WRANGE)
PAIRS = [(i, j) for i in range(N) for j in range(i, N)]
TOP = 8


def lanes():
    return lax.broadcasted_iota(jnp.int32, (8, 128), 1)


def rows():
    return lax.broadcasted_iota(jnp.int32, (8, 128), 0)


def splat_row(m, k):
    return jnp.broadcast_to(m[k : k + 1, :], (8, 128))


def splat_col(m, k):
    return jnp.broadcast_to(m[:, k : k + 1], (8, 128))


def row_sum(m):
    return jnp.broadcast_to(jnp.sum(m, axis=1, keepdims=True), (8, 128))


def shift(m, amount):
    amount = amount % 128
    return pltpu.roll(m, amount, 1) if amount else m


def columns(m, base=0):
    return [splat_col(m, base + k) for k in range(N)]


def columns_t(m):
    same = lanes() == rows()
    return [row_sum(jnp.where(same, splat_row(m, k), 0.0)) for k in range(N)]


def times(cols, m):
    terms = [cols[k] * splat_row(m, k) for k in range(N)]
    while len(terms) > 1:
        terms = [a + b for a, b in zip(terms[::2], terms[1::2])]
    return terms[0]


def solve(cols, rights):
    cols = list(cols)
    row_id = rows()
    for k in range(N):
        here = row_id == k
        inverse = 1.0 / splat_row(cols[k], k)
        factor = cols[k] * inverse

        def step(m):
            line = splat_row(m, k)
            return jnp.where(here, line * inverse, m - factor * line)

        cols = cols[: k + 1] + [step(c) for c in cols[k + 1 :]]
        rights = [step(r) for r in rights]
    return rights


def kernel(
    sizes,
    x_ref,
    w_ref,
    X1,
    R1,
    D2,
    A2,
    T,
    V,
    Q,
    S,
    TA,
    W,
    PX,
    WW,
    WE,
    R,
    PP,
    LPP,
    PQ,
    LPQ,
    G,
    GW,
    ARS,
    ARL,
    load_sem,
    send1,
    recv1,
    send2,
    recv2,
    ar_send,
    ar_recv,
):
    names = ("gx", "gy", "gz")
    nx, ny, nz = sizes
    me = tuple(lax.axis_index(n) for n in names)

    def exists(d):
        cond = None
        for pos, step, count in zip(me, d, sizes):
            term = None
            if step > 0:
                term = pos < count - 1
            elif step < 0:
                term = pos > 0
            if term is not None:
                cond = term if cond is None else cond & term
        return cond

    def opposite(d):
        return tuple(-t for t in d)

    def target(d):
        return tuple(pos + step for pos, step in zip(me, d))

    groups = ((1,), (0, 2))
    offsets = (
        [(0, p, 0) for p in range(1, ny)],
        [(p, 0, r) for p in range(nx) for r in range(nz) if p or r],
    )
    own_slot = (me[1], ny + me[0] * nz + me[2])
    slots = ((0, ny), (ny, nx * nz))

    def peer(d):
        return tuple(lax.rem(pos + p, n) if p else pos for pos, p, n in zip(me, d, sizes))

    load_x = pltpu.make_async_copy(x_ref, V.at[:, pl.ds(1, 16), pl.ds(TOP, 32)], load_sem.at[0])
    load_w = pltpu.make_async_copy(w_ref, W.at[:, pl.ds(1, 16), pl.ds(TOP, 32)], load_sem.at[1])
    load_x.start()
    load_w.start()

    zero = jnp.zeros((8, 128), F32)

    def clear_padded(buf, first, last):
        for field in range(buf.shape[0]):
            for plane in (first, last):
                if plane is not None:
                    for t in range(6):
                        buf[field, plane, pl.ds(8 * t, 8)] = zero

        def body(p, carry):
            for field in range(buf.shape[0]):
                buf[field, p, pl.ds(0, 8)] = zero
                buf[field, p, pl.ds(40, 8)] = zero
            return carry

        lax.fori_loop(1, 17, body, 0)

    clear_padded(V, 0, 17)
    clear_padded(Q, 0, 17)
    clear_padded(W, 0, None)

    def clear_landing(i, carry):
        for t in range(6):
            for s in range(2):
                for k in range(2):
                    LPP[s, k, i, pl.ds(8 * t, 8)] = zero
                LPQ[s, i, pl.ds(8 * t, 8)] = zero
        return carry

    lax.fori_loop(0, 4, clear_landing, 0)

    barrier = pltpu.get_barrier_semaphore()
    for d in DIRS:

        @pl.when(exists(d))
        def _():
            pl.semaphore_signal(
                barrier, inc=1, device_id=target(d), device_id_type=pl.DeviceIdType.MESH
            )

    for step in range(2):
        for d in offsets[step]:
            pl.semaphore_signal(
                barrier, inc=1, device_id=peer(d), device_id_type=pl.DeviceIdType.MESH
            )
    span = []
    for pos, count in zip(me, sizes):
        span.append(1 + (pos > 0).astype(jnp.int32) + (pos < count - 1).astype(jnp.int32))
    def along(step, whole, plus, minus):
        if step == 0:
            return (pl.ds(*whole), pl.ds(*whole))
        src, dst = plus if step > 0 else minus
        return (pl.ds(src, 1), pl.ds(dst, 1))

    def field_part(d, buf, sends, recvs):
        i = DIRS.index(d)
        xs, xd = along(d[0], (1, 16), (16, 0), (1, 17))
        ys, yd = along(d[1], (TOP, 32), (TOP + 31, TOP - 1), (TOP, TOP + 32))
        return pltpu.make_async_remote_copy(
            src_ref=buf.at[:, xs, ys],
            dst_ref=buf.at[:, xd, yd],
            send_sem=sends.at[i],
            recv_sem=recvs.at[i],
            device_id=target(d),
            device_id_type=pl.DeviceIdType.MESH,
        )

    def weight_part(d):
        i = 26 + WDIRS.index((d[0], d[1]))
        k0, kn = WRANGE[(d[0], d[1])]
        xs, xd = along(d[0], (1, 16), (16, 0), (1, 17))
        ys, yd = along(d[1], (TOP, 32), (TOP + 31, TOP - 1), (TOP, TOP + 32))
        return pltpu.make_async_remote_copy(
            src_ref=W.at[pl.ds(k0, kn), xs, ys],
            dst_ref=W.at[pl.ds(k0, kn), xd, yd],
            send_sem=send1.at[i],
            recv_sem=recv1.at[i],
            device_id=target(d),
            device_id_type=pl.DeviceIdType.MESH,
        )

    def column_part(d, both):
        i = DIRS.index(d)
        side = 0 if d[2] > 0 else 1
        if d[0] == 0:
            gs, gd = pl.ds(0, 2), pl.ds(1, 2)
        elif d[0] > 0:
            gs, gd = pl.ds(1, 1), pl.ds(0, 1)
        else:
            gs, gd = pl.ds(0, 1), pl.ds(3, 1)
        if d[1] == 0:
            ys, yd = pl.ds(0, 32), pl.ds(TOP, 32)
        elif d[1] > 0:
            ys, yd = pl.ds(31, 1), pl.ds(TOP - 1, 1)
        else:
            ys, yd = pl.ds(0, 1), pl.ds(TOP + 32, 1)
        src = PP.at[:, gs, ys] if both else PQ.at[gs, ys]
        dst = LPP.at[side, :, gd, yd] if both else LPQ.at[side, gd, yd]
        return pltpu.make_async_remote_copy(
            src_ref=src,
            dst_ref=dst,
            send_sem=(send1 if both else send2).at[i],
            recv_sem=(recv1 if both else recv2).at[i],
            device_id=target(d),
            device_id_type=pl.DeviceIdType.MESH,
        )

    def start_if(d, copy):
        @pl.when(exists(d))
        def _():
            copy.start()

    def recv_if(d, copy):
        @pl.when(exists(opposite(d)))
        def _():
            copy.wait_recv()

    def sent_if(d, copy):
        @pl.when(exists(d))
        def _():
            copy.wait_send()

    flat = sorted((d for d in DIRS if d[2] == 0), key=lambda d: abs(d[1]))
    flat_w = [(a, b, 0) for a, b in WDIRS]
    cols = [d for d in DIRS if d[2] != 0]

    lane = lanes()
    odd = lax.rem(lane, 2) == 1
    first = lane == 0
    last = lane == 127
    half = lane // 2

    def gather_columns(fields):
        total = zero
        for slot, v in enumerate(fields):
            total = jnp.where(half == slot, shift(v, 2 * slot + 1), total)
        return total

    def merge_columns(dst):
        for xg in range(2):
            for t in range(4):
                at = pl.ds(8 * t, 8)
                parts = [
                    jnp.where(lane // 16 == xm, shift(PX[xg * 8 + xm, at], 16 * xm), 0.0)
                    for xm in range(8)
                ]
                while len(parts) > 1:
                    parts = [a + b for a, b in zip(parts[::2], parts[1::2])]
                dst(xg, at, parts[0])

    def pack(dst, group):
        def body(i, carry):
            for k in range(4):
                x = 4 * i + k
                for t in range(4):
                    PX[x, pl.ds(8 * t, 8)] = gather_columns(
                        group(x + 1, pl.ds(TOP + 8 * t, 8))
                    )
            return carry

        lax.fori_loop(0, 4, body, 0)
        merge_columns(dst)

    def put_weights(xg, at, total):
        PP[1, xg, at] = total

    def weight_group(p, at):
        return [jnp.where(first, W[UP[j], p, at], W[LOW[j], p, at]) for j in range(5)]

    def unpack(get, dst, planes):
        for t in range(6):
            r0 = 8 * t
            merged = {}
            for xi in planes:
                if xi == 0:
                    g, off = 0, 112
                elif xi == 17:
                    g, off = 3, 0
                else:
                    g, off = 1 + (xi - 1) // 8, 16 * ((xi - 1) % 8)
                if g not in merged:
                    merged[g] = jnp.where(odd, get(1, g, r0), get(0, g, r0))
                dst[xi, pl.ds(r0, 8)] = shift(merged[g], -off)

    def blocks(body, first_x, count, width):
        def several(i, carry):
            for k in range(width):
                body(first_x + width * i + k, carry)
            return carry

        lax.fori_loop(0, count, several, 0)

    flat_y = [d for d in flat if d[0] == 0]
    flat_x = [d for d in flat if d[0] != 0]
    flat_wy = [d for d in flat_w if d[0] == 0]
    flat_wx = [d for d in flat_w if d[0] != 0]
    cols_y = [d for d in cols if d[0] == 0]
    cols_x = [d for d in cols if d[0] != 0]

    def put_pp(xg, at, total):
        PP[0, xg, at] = total

    load_x.wait()
    pack(put_pp, lambda p, at: [V[f, p, at] for f in range(N)])
    load_w.wait()
    pack(put_weights, weight_group)

    pl.semaphore_wait(
        barrier, span[0] * span[1] * span[2] - 1 + (ny - 1) + (nx * nz - 1)
    )

    for d in flat_y:
        start_if(d, field_part(d, V, send1, recv1))
    for d in flat_wy:
        start_if(d, weight_part(d))
    for d in cols_y:
        start_if(d, column_part(d, True))
    for d in flat_x:
        start_if(d, field_part(d, V, send1, recv1))
    for d in cols_x:
        start_if(d, column_part(d, True))
    for d in flat_wx:
        start_if(d, weight_part(d))

    def m_of(a, b):
        return 3 * (a + 1) + (b + 1)

    def spread_columns(v, even_from, odd_from):
        return jnp.take_along_axis(v, jnp.where(odd, odd_from, even_from), axis=1)

    def prepare_own(x, carry):
        for t in range(4):
            out = pl.ds(8 * t, 8)
            own = [W[k, x + 1, pl.ds(TOP + 8 * t, 8)] for k in range(14)]
            diag = (own[0] + own[1]) + (own[2] + own[3])
            for k in range(4, 14, 2):
                diag = diag + (own[k] + own[k + 1])
            WW[0, x, out] = diag
            for j, (a, b) in enumerate(SLOTS):
                WW[1 + j, x, out] = shift(own[LOW[j]], 1)
                if j:
                    WW[5 + j, x, out] = shift(own[UP[j]], 127)
                    WE[m_of(a, b), x, out] = spread_columns(
                        jnp.where(first, own[UP[j]], own[LOW[j]]), 0, 127
                    )
        return carry

    def prepare(x, carry):
        for t in range(4):
            r0 = TOP + 8 * t

            def w_at(k, a=0, b=0):
                return W[k, x + 1 + a, pl.ds(r0 + b, 8)]

            out = pl.ds(8 * t, 8)
            diag = WW[0, x, out]
            ahead = zero
            behind = w_at(LOW[0])
            own = spread_columns(
                jnp.where(last, behind, GW[x + 1, pl.ds(r0, 8)]), 0, 127
            )
            WE[m_of(0, 0), x, out] = own
            edge = jnp.where(odd, 0.0, own)
            for j, (a, b) in enumerate(SLOTS):
                if j == 0:
                    continue
                back = spread_columns(GW[x + 1 - a, pl.ds(r0 - b, 8)], 2 * j, 2 * j + 1)
                WE[m_of(-a, -b), x, out] = back
                edge = edge + back
                diag = diag + w_at(INDEX[(a, b, 0)], -a, -b)
                ahead = ahead + w_at(UP[j], -a, -b)
                behind = behind + w_at(LOW[j], -a, -b)
            diag = diag + jnp.where(last, edge, shift(ahead, 127))
            diag = diag + jnp.where(first, edge, shift(behind, 1))
            WW[0, x, out] = diag
        return carry

    blocks(prepare_own, 0, 8, 2)

    def gram_loop(get):
        sums = []
        for lo, hi in ((0, 3), (3, N)):
            pairs = [(i, j) for i, j in PAIRS if lo <= i < hi]

            def body(planes, acc):
                acc = list(acc)
                for k in range(8):
                    x, t = 2 * planes + k // 4, k % 4
                    left, right = get(x, t, range(lo, hi), range(lo, N))
                    for n, (i, j) in enumerate(pairs):
                        acc[n] = acc[n] + left[i] * right[j]
                return tuple(acc)

            sums += list(lax.fori_loop(0, 8, body, tuple(zero for _ in pairs)))
        return sums

    def spread(parts, acc, offset):
        for n, (i, j) in enumerate(PAIRS):
            total = row_sum(acc[n])
            parts[i] = jnp.where(lane == offset + j, total, parts[i])
            if i != j:
                parts[j] = jnp.where(lane == offset + i, total, parts[j])
        return parts

    def fold(parts):
        result = zero
        for i in range(N):
            total = jnp.broadcast_to(jnp.sum(parts[i], axis=0, keepdims=True), (8, 128))
            result = jnp.where(rows() == i, total, result)
        return result

    def row(buf, f, x, t):
        return buf[f, x + 1, pl.ds(TOP + 8 * t, 8)]

    def get_rr(x, t, left, right):
        v = {f: row(V, f, x, t) for f in right}
        return v, v

    parts1 = spread([zero] * N, gram_loop(get_rr), 0)

    for d in flat_y:
        recv_if(d, field_part(d, V, send1, recv1))
    for d in flat_wy:
        recv_if(d, weight_part(d))
    for d in cols_y:
        recv_if(d, column_part(d, True))

    def get_lpp(k):
        return lambda s, g, r0: LPP[s, k, g, pl.ds(r0, 8)]

    def get_lpq(s, g, r0):
        return LPQ[s, g, pl.ds(r0, 8)]

    unpack(get_lpp(0), G, range(1, 17))
    unpack(get_lpp(1), GW, range(1, 17))

    def edges(x, carry):
        for t in range(4):
            total = zero
            for a, b in PLANE:
                total = total + WE[m_of(a, b), x, pl.ds(8 * t, 8)] * G[
                    x + 1 + a, pl.ds(TOP + 8 * t + b, 8)
                ]
            R[x, pl.ds(8 * t, 8)] = total
        return carry

    def coupling(x, t, a, b, c):
        j = SLOTS.index((a, b)) if (a, b) in SLOTS else SLOTS.index((-a, -b))
        here = pl.ds(8 * t, 8)
        away = W.at[:, x + 1 + a, pl.ds(TOP + 8 * t + b, 8)]
        ahead = (a, b) in SLOTS
        if c == 0:
            if (a, b) == (0, 0):
                return WW[0, x, here]
            if ahead:
                return W[INDEX[(a, b, 0)], x + 1, pl.ds(TOP + 8 * t, 8)]
            return away[INDEX[(-a, -b, 0)]]
        if c == 1:
            return WW[1 + j, x, here] if ahead else away[UP[j]]
        if ahead and j:
            return WW[5 + j, x, here]
        return away[LOW[j]]

    def operate(src, put):
        def body(x, carry):
            for t in range(4):
                halo = R[x, pl.ds(8 * t, 8)]
                for group in (range(0, 4), range(4, N)):
                    centre = {}
                    sums = {f: [None, None, None] for f in group}
                    for a, b in PLANE:
                        weights = [coupling(x, t, a, b, c) for c in (0, 1, -1)]
                        for f in group:
                            v = src[f, x + 1 + a, pl.ds(TOP + 8 * t + b, 8)]
                            for c in range(3):
                                term = weights[c] * v
                                if c == 0 and (a, b) == (0, 0):
                                    centre[f] = term
                                elif sums[f][c] is None:
                                    sums[f][c] = term
                                else:
                                    sums[f][c] = sums[f][c] + term
                    for f in group:
                        side = shift(halo, -(2 * f + 1))
                        total = centre[f] - sums[f][0]
                        total = total - shift(jnp.where(first, side, sums[f][1]), 127)
                        total = total - shift(jnp.where(last, side, sums[f][2]), 1)
                        put(f, x, t, total)
            return carry

        return body

    def ends(body):
        lax.fori_loop(0, 2, lambda i, carry: body(15 * i, carry), 0)

    def put_q(f, x, t, value):
        Q[f, x + 1, pl.ds(TOP + 8 * t, 8)] = value

    def put_s(f, x, t, value):
        S[f, x, pl.ds(8 * t, 8)] = value

    blocks(prepare, 1, 5, 3)
    blocks(edges, 1, 7, 2)
    blocks(operate(V, put_q), 1, 14, 1)
    for d in flat_x:
        recv_if(d, field_part(d, V, send1, recv1))
    for d in flat_wx:
        recv_if(d, weight_part(d))
    for d in cols_x:
        recv_if(d, column_part(d, True))
    unpack(get_lpp(0), G, (0, 17))
    unpack(get_lpp(1), GW, (0,))
    prepare(0, 0)
    ends(edges)
    ends(operate(V, put_q))

    for d in flat_y + flat_x:
        start_if(d, field_part(d, Q, send2, recv2))

    def put_pq(xg, at, total):
        PQ[xg, at] = total

    pack(put_pq, lambda p, at: [Q[f, p, at] for f in range(N)])
    for d in cols_y + cols_x:
        start_if(d, column_part(d, False))

    def reduce_copies(which, step):
        copies = []
        for i, d in enumerate(offsets[step]):
            i = slots[step][0] + i
            copies.append(
                pltpu.make_async_remote_copy(
                    src_ref=ARS.at[which, step],
                    dst_ref=ARL.at[which, own_slot[step]],
                    send_sem=ar_send.at[which, i],
                    recv_sem=ar_recv.at[which, i],
                    device_id=peer(d),
                    device_id_type=pl.DeviceIdType.MESH,
                )
            )
        return copies

    def reduce_start(which, step, value):
        ARS[which, step] = value
        ARL[which, own_slot[step]] = value
        for copy in reduce_copies(which, step):
            copy.start()

    def reduce_finish(which, step):
        for copy in reduce_copies(which, step):
            copy.wait_recv()
        lo, count = slots[step]
        parts = [ARL[which, lo + i] for i in range(count)]
        while len(parts) > 1:
            parts = [a + b for a, b in zip(parts[::2], parts[1::2])]
        return parts[0]

    def get_rq(x, t, left, right):
        return (
            {f: row(V, f, x, t) for f in left},
            {f: row(Q, f, x, t) for f in right},
        )

    def get_qq(x, t, left, right):
        q = {f: row(Q, f, x, t) for f in right}
        return q, q

    parts1 = spread(parts1, gram_loop(get_rq), 8)
    reduce_start(0, 0, fold(parts1))
    reduce_start(2, 0, fold(spread([zero] * N, gram_loop(get_qq), 0)))

    for d in flat_y:
        recv_if(d, field_part(d, Q, send2, recv2))
    for d in cols_y:
        recv_if(d, column_part(d, False))
    unpack(get_lpq, G, range(1, 17))
    blocks(edges, 1, 7, 2)
    blocks(operate(Q, put_s), 1, 4, 1)
    reduce_start(0, 1, reduce_finish(0, 0))
    reduce_start(2, 1, reduce_finish(2, 0))
    blocks(operate(Q, put_s), 5, 10, 1)
    for d in flat_x:
        recv_if(d, field_part(d, Q, send2, recv2))
    for d in cols_x:
        recv_if(d, column_part(d, False))
    unpack(get_lpq, G, (0, 17))
    ends(edges)
    ends(operate(Q, put_s))
    sum1 = reduce_finish(0, 1)

    def trace(m):
        total = row_sum(jnp.where(lane == rows(), m, 0.0))
        return jnp.broadcast_to(jnp.sum(total, axis=0, keepdims=True), (8, 128))

    small = lane < 8
    own_gram = jnp.where(small, sum1, 0.0)
    g1 = jnp.where(small, shift(sum1, -8), 0.0)
    theta = trace(g1) / trace(own_gram)
    h1 = g1 - theta * own_gram

    def moved(f, x, t):
        return row(Q, f, x, t) - theta * row(V, f, x, t)

    def get_h2(x, t, left, right):
        z = {f: moved(f, x, t) for f in right}
        return z, z

    def get_zs(x, t, left, right):
        return (
            {f: moved(f, x, t) for f in left},
            {f: S[f, x, pl.ds(8 * t, 8)] for f in right},
        )

    parts2 = [zero] * N
    parts2 = spread(parts2, gram_loop(get_h2), 0)
    parts2 = spread(parts2, gram_loop(get_zs), 8)
    reduce_start(1, 0, fold(parts2))

    unit = jnp.where(lane == rows(), 1.0, 0.0)
    g2 = reduce_finish(2, 1)
    g1_cols, h1_cols = columns(g1), columns(h1)
    alpha, rest = solve(g1_cols, [own_gram, h1])
    alpha_t, rest_t = columns_t(alpha), columns_t(rest)
    beta = own_gram - times(g1_cols, alpha)
    beta = beta + times(alpha_t, times(columns(g2), alpha) - g1)
    own_cols = columns(own_gram)
    (beta,) = solve(own_cols, [beta])
    mix = rest + beta
    mix_t = columns_t(mix)
    g1_mix = times(g1_cols, mix)
    early = times(own_cols, rest) - times(h1_cols, alpha)
    early = times(rest_t, early) - times(alpha_t, times(h1_cols, rest))

    def put_table(dst, base, m):
        for i in range(N):
            line = splat_row(m, i)
            for j in range(N):
                dst[base + N * j + i] = splat_col(line, j)

    put_table(TA, 0, alpha)
    put_table(TA, 64, unit + beta)

    def second_body(j, carry):
        a = [TA[N * j + i] for i in range(N)]
        b = [TA[64 + N * j + i] for i in range(N)]

        def body(x, carry):
            for t in range(4):
                at = pl.ds(8 * t, 8)
                r = [row(V, f, x, t) for f in range(N)]
                q = [row(Q, f, x, t) for f in range(N)]
                s = [S[f, x, at] for f in range(N)]

                def comb(c, v):
                    total = c[0] * v[0]
                    for i in range(1, N):
                        total = total + c[i] * v[i]
                    return total

                aq = comb(a, q)
                X1[j, x, at] = comb(a, r)
                R1[j, x, at] = row(V, j, x, t) - aq
                D2[j, x, at] = comb(b, r) - aq
                A2[j, x, at] = comb(b, q) - comb(a, s)
            return carry

        lax.fori_loop(0, 16, body, 0)
        return carry

    lax.fori_loop(0, 2, second_body, 0)
    reduce_start(1, 1, reduce_finish(1, 0))
    lax.fori_loop(2, N, second_body, 0)
    for d in flat:
        sent_if(d, field_part(d, V, send1, recv1))
        sent_if(d, field_part(d, Q, send2, recv2))
    for d in flat_w:
        sent_if(d, weight_part(d))
    for d in cols:
        sent_if(d, column_part(d, True))
        sent_if(d, column_part(d, False))
    for which in (0, 2):
        for copy in reduce_copies(which, 0) + reduce_copies(which, 1):
            copy.wait_send()
    sum2 = reduce_finish(1, 1)

    h2_cols, zs_cols = columns(sum2), columns(sum2, 8)
    norm_next = early + times(alpha_t, times(h2_cols, alpha))
    cross = [h + theta * g for h, g in zip(h2_cols, h1_cols)]
    h3_cols = [z - theta * c for z, c in zip(zs_cols, cross)]
    curve = times(mix_t, g1_mix - times(cross, alpha)) + times(
        alpha_t, times(h3_cols, alpha) - times(cross, mix)
    )
    (alpha2,) = solve(columns(curve), [norm_next])
    put_table(T, 0, alpha2)

    for copy in reduce_copies(1, 0) + reduce_copies(1, 1):
        copy.wait_send()


def finish_kernel(X1, R1, D2, A2, T, x_out, r_out, X, Y, sems):
    def store(j, lo, count):
        at = pl.ds(lo, count)
        return [
            pltpu.make_async_copy(
                buf.at[j, at], out.at[j, at], sems.at[k, j + lo // 4]
            )
            for k, (buf, out) in enumerate(((X, x_out), (Y, r_out)))
        ]

    started = []
    for pair in range(0, N, 2):
        js = (pair, pair + 1)
        a = {j: [T[N * j + i] for i in range(N)] for j in js}

        def body(planes, carry):
            for k in range(8):
                p = 2 * planes + k // 4
                at = pl.ds(8 * (k % 4), 8)
                d = [D2[i, p, at] for i in range(N)]
                e = [A2[i, p, at] for i in range(N)]
                for j in js:
                    x = X1[j, p, at]
                    res = R1[j, p, at]
                    for i in range(0, N, 2):
                        x = x + (a[j][i] * d[i] + a[j][i + 1] * d[i + 1])
                        res = res - (a[j][i] * e[i] + a[j][i + 1] * e[i + 1])
                    X[j, p, at] = x
                    Y[j, p, at] = res
            return carry

        for lo, count in ((0, 16),) if pair < 6 else ((0, 8), (8, 8)):
            lax.fori_loop(lo // 2, (lo + count) // 2, body, 0)
            for j in js:
                for copy in store(j, lo, count):
                    copy.start()
                    started.append(copy)
    for copy in started:
        copy.wait()


def shards(sizes, rhs, stencil):
    nx, ny, nz = sizes
    block = rhs.shape
    anyspace = pl.BlockSpec(memory_space=pl.ANY)
    local = pl.BlockSpec(memory_space=pltpu.VMEM)
    hbm = pl.BlockSpec(memory_space=pltpu.HBM)
    field = jax.ShapeDtypeStruct(block, F32)
    kept = pl.pallas_call(
        functools.partial(kernel, sizes),
        out_shape=(field,) * 4 + (jax.ShapeDtypeStruct((64, 8, 128), F32),),
        in_specs=[hbm, hbm],
        out_specs=(local,) * 5,
        scratch_shapes=[
            pltpu.VMEM((8, 18, 48, 128), F32),
            pltpu.VMEM((8, 18, 48, 128), F32),
            pltpu.VMEM(block, F32),
            pltpu.VMEM((128, 8, 128), F32),
            pltpu.VMEM((14, 17, 48, 128), F32),
            pltpu.VMEM((16, 32, 128), F32),
            pltpu.VMEM((10, 16, 32, 128), F32),
            pltpu.VMEM((9, 16, 32, 128), F32),
            pltpu.VMEM((16, 32, 128), F32),
            pltpu.VMEM((2, 2, 32, 128), F32),
            pltpu.VMEM((2, 2, 4, 48, 128), F32),
            pltpu.VMEM((2, 32, 128), F32),
            pltpu.VMEM((2, 4, 48, 128), F32),
            pltpu.VMEM((18, 48, 128), F32),
            pltpu.VMEM((17, 48, 128), F32),
            pltpu.VMEM((3, 2, 8, 128), F32),
            pltpu.VMEM((3, ny + nx * nz, 8, 128), F32),
            pltpu.SemaphoreType.DMA((2,)),
            pltpu.SemaphoreType.DMA((31,)),
            pltpu.SemaphoreType.DMA((31,)),
            pltpu.SemaphoreType.DMA((26,)),
            pltpu.SemaphoreType.DMA((26,)),
            pltpu.SemaphoreType.DMA((3, ny + nx * nz)),
            pltpu.SemaphoreType.DMA((3, ny + nx * nz)),
        ],
        compiler_params=pltpu.CompilerParams(
            collective_id=0, has_side_effects=True, vmem_limit_bytes=44 * 2**20
        ),
        name="operator",
    )(rhs, stencil)
    return pl.pallas_call(
        finish_kernel,
        out_shape=(jax.ShapeDtypeStruct(block, F32), jax.ShapeDtypeStruct(block, F32)),
        in_specs=[local] * 5,
        out_specs=(anyspace, anyspace),
        scratch_shapes=[
            pltpu.VMEM(block, F32),
            pltpu.VMEM(block, F32),
            pltpu.SemaphoreType.DMA((2, N + 2)),
        ],
        compiler_params=pltpu.CompilerParams(vmem_limit_bytes=24 * 2**20),
        name="finish",
    )(*kept)


def solution(mesh):
    sizes = tuple(mesh.shape[n] for n in ("gx", "gy", "gz"))
    placed = P(None, "gx", "gy", "gz")
    return jax.shard_map(
        functools.partial(shards, sizes),
        mesh=mesh,
        in_specs=(placed, placed),
        out_specs=(placed, placed),
        check_vma=False,
    )
```
